32 devices in a mesh: groups: 2 (over y), gx: 4 (over z), gy: 2 (over x), gz: 2 (over core).
Axes of the slice: x: 2, y: 2, z: 4, core: 2. Of those that a mesh axis runs over, the one named last changes fastest.
Arguments:
- latents: bfloat16 [8, 2, 2, 128, 128], P(('groups', 'gx'), 'gy', 'gz'), parts along dimension 0, may hold values from -6 to 6
- offsets: bfloat16 [8, 2, 2, 3, 128], P(('groups', 'gx'), 'gy', 'gz'), parts along dimension 0, may hold values from 0 to 1
- neighbours: int32 [8, 2, 2, 384], P(('groups', 'gx'), 'gy', 'gz'), parts along dimension 0, may hold values from 0 to 2047, as said below
- counts: int32 [8, 2, 2], P(('groups', 'gx'), 'gy', 'gz'), parts along dimension 0, may hold values from 1 to 384, as said below
- w_recv: bfloat16 [1, 128, 128], replicated, may hold values from -0.5 to 0.5
- w_send: bfloat16 [1, 128, 128], replicated, may hold values from -0.5 to 0.5
- w_rel: bfloat16 [1, 4, 128], replicated, may hold values from -3 to 3
- b_first: float32 [1, 128], replicated, may hold values from -5 to 5
- w_edge: bfloat16 [1, 128, 128], replicated, may hold values from -0.5 to 0.5
- b_edge: float32 [1, 128], replicated, may hold values from -5 to 5
- w_self: bfloat16 [1, 128, 128], replicated, may hold values from -0.5 to 0.5
- w_agg: bfloat16 [1, 128, 128], replicated, may hold values from -0.5 to 0.5
- w_out: bfloat16 [1, 128, 128], replicated, may hold values from -0.5 to 0.5
- norm_gain: float32 [1, 128], replicated, may hold values from 0.1 to 1.9
Outputs:
- processed: bfloat16 [8, 2, 2, 128, 128], P(('groups', 'gx'), 'gy', 'gz'), parts along dimension 0
The draws below stay inside these ranges and needn't reach their ends.
There are 2 independent parts, one for each index of `groups`. The reference program is written for one: setup_inputs(seed, part) draws one part's arguments, and reference() takes and returns one part's arrays. A program takes and returns all parts, laid end to end along the dimension named above; an argument that names none is the same for every part. Nothing has to cross between parts.
Inputs may be any that keep to these rules, and one draw needn't show every extreme that they name: `neighbours`: each sender is a particle of the same cell or of a cell whose three coordinates differ from the receiver cell's by at most one. Only the first counts[cell] senders of a cell are live, the rest is padding. In the cells whose first coordinate is below 1 all 384 senders are live.
All inputs are finite; a program needn't handle non-finite values.
Results may differ from the reference program's by a relative error of at most 0.0055.
Values may be sent and summed in bfloat16 or wider, within the bound.
A program may use at most 64 MiB of HBM per device.

```python
import jax
import jax.numpy as jnp
from jax import lax

W = 128
SLOTS = 128
NBLK = 3
STEPS = 1
NX = 4
NY = 2
NZ = 2


def draw_neighbours(key, part):
    draw_shape = (NX, NY, NZ, NBLK * SLOTS)
    subkeys = jax.random.split(jax.random.fold_in(key, 11), 4)
    axis_x = jnp.arange(NX, dtype=jnp.int32)[:, None, None, None]
    axis_y = jnp.arange(NY, dtype=jnp.int32)[None, :, None, None]
    axis_z = jnp.arange(NZ, dtype=jnp.int32)[None, None, :, None]
    coord_x = jnp.clip(axis_x + jax.random.randint(subkeys[0], draw_shape, -1, 2), 0, NX - 1)
    coord_y = jnp.clip(axis_y + jax.random.randint(subkeys[1], draw_shape, -1, 2), 0, NY - 1)
    coord_z = jnp.clip(axis_z + jax.random.randint(subkeys[2], draw_shape, -1, 2), 0, NZ - 1)
    slot_pick = jax.random.randint(subkeys[3], draw_shape, 0, SLOTS)
    return (((coord_x * NY + coord_y) * NZ + coord_z) * SLOTS + slot_pick).astype(jnp.int32)


def draw_counts(key, part):
    axis_x = jnp.arange(NX, dtype=jnp.int32)[:, None, None]
    sparse = jax.random.randint(jax.random.fold_in(key, 23), (NX, NY, NZ), 1, SLOTS + 1)
    packed = jnp.full((NX, NY, NZ), NBLK * SLOTS, jnp.int32)
    return jnp.where(axis_x < NX // 4, packed, sparse).astype(jnp.int32)


def levels(key, extent, pieces, smallest, largest):
    loudness, own = 1.0, jax.random.fold_in(key, 6)
    for axis_at, shards_of in pieces:
        draws = jnp.exp(jax.random.uniform(jax.random.fold_in(own, axis_at), (shards_of,), jnp.float32, smallest / len(pieces), largest / len(pieces)))
        loudness = loudness * jnp.repeat(draws, extent[axis_at] // shards_of).reshape([-1 if axis == axis_at else 1 for axis in range(len(extent))])
    return loudness


def scatter_about(own_key, dims, width, limit, shards=(), kind=jnp.bfloat16):
    factor_of = levels(own_key, dims, shards, -0.22, 0.18) if shards else 1.0
    values = jax.random.normal(own_key, dims, jnp.float32) * width * factor_of
    return jnp.minimum(jnp.maximum(values, -limit), limit).astype(kind)


def setup_inputs(seed: int = 0, part: int = 0) -> dict:
    arg_keys = jax.random.split(jax.random.key(seed), 15)
    own_keys = jax.random.split(jax.random.fold_in(arg_keys[14], part), 15)
    latents = scatter_about(own_keys[0], (NX, NY, NZ, SLOTS, W), 1.0, 6.0, ((0, 4), (1, 2), (2, 2)))
    offsets = jnp.clip(1.0 * jax.random.uniform(own_keys[1], (NX, NY, NZ, 3, SLOTS), jnp.float32) ** levels(own_keys[1], (NX, NY, NZ, 3, SLOTS), ((0, 4), (1, 2), (2, 2)), -0.2, 0.2), 0.0, 1.0).astype(jnp.bfloat16)
    neighbours = draw_neighbours(jax.random.fold_in(jax.random.fold_in(arg_keys[14], part), 71), part)
    counts = draw_counts(jax.random.fold_in(jax.random.fold_in(arg_keys[14], part), 71), part)
    w_recv = scatter_about(arg_keys[4], (STEPS, W, W), W ** -0.5, 0.5)
    w_send = scatter_about(arg_keys[5], (STEPS, W, W), W ** -0.5, 0.5)
    w_rel = scatter_about(arg_keys[6], (STEPS, 4, W), 4 ** -0.5, 3.0)
    b_first = scatter_about(arg_keys[7], (STEPS, W), 1.0, 5.0, (), jnp.float32)
    w_edge = scatter_about(arg_keys[8], (STEPS, W, W), W ** -0.5, 0.5)
    b_edge = scatter_about(arg_keys[9], (STEPS, W), 1.0, 5.0, (), jnp.float32)
    w_self = scatter_about(arg_keys[10], (STEPS, W, W), W ** -0.5, 0.5)
    w_agg = scatter_about(arg_keys[11], (STEPS, W, W), W ** -0.5, 0.5)
    w_out = scatter_about(arg_keys[12], (STEPS, W, W), W ** -0.5, 0.5)
    norm_gain = jnp.clip(1.0 + 0.18 * jax.random.normal(arg_keys[13], (STEPS, W), jnp.float32), 0.1, 1.9)
    return {"latents": latents, "offsets": offsets, "neighbours": neighbours, "counts": counts, "w_recv": w_recv, "w_send": w_send, "w_rel": w_rel, "b_first": b_first, "w_edge": w_edge, "b_edge": b_edge, "w_self": w_self, "w_agg": w_agg, "w_out": w_out, "norm_gain": norm_gain}


def edge_sum(recv_term, send_term, recv_place, send_place, live_mask, rel_weight, w_edge, b_edge):
    row_count, latent_width = recv_term.shape
    tile_rows = min(16, row_count)
    tile_count = row_count // tile_rows

    def tile_messages(operands):
        recv_tile, place_tile = operands
        relative = send_place[:, None, :] - place_tile[:, :, None]
        features = jnp.concatenate([relative, 0.25 * lax.optimization_barrier(jnp.sum(relative * relative, axis=0, keepdims=True))], axis=0)
        place_term = jnp.einsum('cij,cw->ijw', features, rel_weight, precision=lax.Precision.HIGHEST)
        pre_act = recv_tile[:, None, :] + send_term[None, :, :] + place_term
        edge_act = jax.nn.silu(pre_act).astype(jnp.bfloat16)
        message = jnp.dot(edge_act.reshape(-1, latent_width), w_edge, preferred_element_type=jnp.float32) + b_edge
        message = jax.nn.silu(message).reshape(tile_rows, -1, latent_width)
        return jnp.einsum('ijw,j->iw', message, live_mask, precision=lax.Precision.HIGHEST)
    recv_tiles = recv_term.reshape(tile_count, tile_rows, latent_width)
    place_tiles = recv_place.reshape(3, tile_count, tile_rows).transpose(1, 0, 2)
    return lax.map(tile_messages, (recv_tiles, place_tiles)).reshape(row_count, latent_width)

def renew(latent, summed, w_self, w_agg, w_out, norm_gain):
    pooled = (summed / latent.shape[0]).astype(jnp.bfloat16)
    hidden = jax.nn.silu(jnp.dot(latent, w_self, preferred_element_type=jnp.float32) + jnp.dot(pooled, w_agg, preferred_element_type=jnp.float32)).astype(jnp.bfloat16)
    result = jnp.dot(hidden, w_out, preferred_element_type=jnp.float32)
    center = lax.optimization_barrier(jnp.mean(result, axis=-1, keepdims=True))
    spread = lax.optimization_barrier(jnp.mean((result - center) ** 2, axis=-1, keepdims=True))
    normed = (result - center) * lax.rsqrt(spread + 1e-05) * norm_gain
    return (latent.astype(jnp.float32) + normed).astype(jnp.bfloat16)

def reference(latents, offsets, neighbours, counts, w_recv, w_send, w_rel, b_first, w_edge, b_edge, w_self, w_agg, w_out, norm_gain):
    cell_count = NX * NY * NZ
    current = latents.reshape(cell_count, SLOTS, W)
    cell_ids = jnp.arange(cell_count, dtype=jnp.int32)
    coords = jnp.stack([cell_ids // (NY * NZ), cell_ids // NZ % NY, cell_ids % NZ], axis=1).astype(jnp.float32)
    places = offsets.reshape(cell_count, 3, SLOTS).astype(jnp.float32) + coords[:, :, None]
    flat_places = places.transpose(1, 0, 2).reshape(3, cell_count * SLOTS)
    neighbour_rows = neighbours.reshape(cell_count, NBLK * SLOTS)
    count_rows = counts.reshape(cell_count)
    slot_ids = jnp.arange(SLOTS, dtype=jnp.int32)
    for step_index in range(STEPS):
        flat_latents = current.reshape(cell_count * SLOTS, W)
        rel_weight = w_rel[step_index].astype(jnp.float32)

        def update_cell(operands, step_index=step_index, flat_latents=flat_latents, rel_weight=rel_weight):
            latent, recv_place, sender_row, sender_count = operands
            recv_term = jnp.dot(latent, w_recv[step_index], preferred_element_type=jnp.float32) + b_first[step_index]
            summed = jnp.zeros((SLOTS, W), jnp.float32)
            for block_index in range(NBLK):
                sender_ids = sender_row[block_index * SLOTS:(block_index + 1) * SLOTS]
                gathered = jnp.take(flat_latents, sender_ids, axis=0)
                send_term = jnp.dot(gathered, w_send[step_index], preferred_element_type=jnp.float32)
                send_place = jnp.take(flat_places, sender_ids, axis=1)
                live_mask = (block_index * SLOTS + slot_ids < sender_count).astype(jnp.float32)
                summed = summed + edge_sum(recv_term, send_term, recv_place, send_place, live_mask, rel_weight, w_edge[step_index], b_edge[step_index])
            return renew(latent, summed, w_self[step_index], w_agg[step_index], w_out[step_index], norm_gain[step_index])
        current = lax.map(update_cell, (current, places, neighbour_rows, count_rows))
    return current.reshape(NX, NY, NZ, SLOTS, W)
```

```python
import functools

import jax
import jax.numpy as jnp
from jax import lax
from jax.experimental import pallas as pl
from jax.experimental.pallas import tpu as pltpu
from jax.sharding import PartitionSpec as P

MESH = pl.DeviceIdType.MESH
AXES = ("gx", "gy", "gz")
PACK = 16
EARLY_GROUP = 16
GROUP = 32
NT = (((1,), (1,)), ((), ()))
f32, bf16 = jnp.float32, jnp.bfloat16


def split(value, size):
    if size & (size - 1) == 0:
        return value >> (size.bit_length() - 1), value & (size - 1)
    return lax.div(value, size), lax.rem(value, size)


def wide(axis):
    return lax.axis_size(axis) > 2


def slots_of(axis):
    return min(lax.axis_size(axis), 3)


def moves(axis):
    size, here = lax.axis_size(axis), lax.axis_index(axis)
    if size == 1:
        return []
    if size == 2:
        return [(1 - here, None)]
    return [(here - 1, here > 0), (here + 1, here < size - 1)]


def slot_on(axis, source, target):
    return source - target + 1 if wide(axis) else source


def both(*conditions):
    held = [c for c in conditions if c is not None]
    return functools.reduce(jnp.logical_and, held) if held else None


def guarded(condition, action):
    if condition is None:
        action()
    else:
        pl.when(condition)(action)


def dot(a, b):
    return jnp.dot(a, b, preferred_element_type=f32)


def dot_nt(a, b):
    return lax.dot_general(a, b, NT, preferred_element_type=f32)


def edges_of(own, near, send, rel_half):
    halves = []
    for n in range(2):
        gap = jnp.transpose(jnp.broadcast_to(near[n : n + 1], (send.shape[1], send.shape[0])))
        pre = (own[n : n + 1] + send) + gap * rel_half
        halves.append(pre * (jnp.tanh(pre) + 1))
    return jnp.concatenate(halves, axis=1)


def messages_of(result, masked):
    width = masked.shape[1]
    half, sums = result.astype(bf16), []
    for n in range(2):
        total = None
        for r in range(0, masked.shape[0], PACK):
            msg = half[r : r + PACK, n * width : (n + 1) * width] + masked[r : r + PACK]
            gate = jnp.tanh(msg) + 1
            term = msg.astype(f32) * gate.astype(f32)
            total = term if total is None else total + term
        sums.append(total[:8] + total[8:])
    return sums


def fold_rows(part, rows):
    total = part[pl.ds(0, rows, stride=8), :]
    for k in range(1, 8):
        total = total + part[pl.ds(k, rows, stride=8), :]
    return total


A_INPUTS = 10
A_OUTPUTS = 7
LOAD_ORDER = (1, 5, 2, 6, 3, 0, 4, 7, 8, 9)


def exchange(*refs):
    hbm, outs = refs[:A_INPUTS], refs[A_INPUTS : A_INPUTS + A_OUTPUTS]
    held = refs[A_INPUTS + A_OUTPUTS : 2 * A_INPUTS + A_OUTPUTS]
    load_sem, table, chosen, part, send_sem, recv_sem = refs[2 * A_INPUTS + A_OUTPUTS :]
    counts_ref, latents_ref, offsets_ref, neighbours_ref, w_recv, w_send, w_rel, b_first, w_edge, b_edge = held
    send_half, near, recv_half, masked, pair_edge, pooled, tally = outs
    loads = [pltpu.make_async_copy(src, dst, load_sem.at[n]) for n, (src, dst) in enumerate(zip(hbm, held))]
    for n in LOAD_ORDER:
        loads[n].start()
    slots, width = latents_ref.shape[3], latents_ref.shape[4]
    senders = neighbours_ref.shape[3]
    blocks, room = senders // slots, senders + slots
    here = [lax.axis_index(axis) for axis in AXES]
    sizes = [lax.axis_size(axis) for axis in AXES]
    spans = [slots_of(axis) for axis in AXES]
    count, span_z = table.shape[0], spans[2]

    def slot(coords):
        return (coords[0] * spans[1] + coords[1]) * spans[2] + coords[2]

    def slot_between(source, target):
        return slot([slot_on(a, s, t) for a, s, t in zip(AXES, source, target)])

    own = slot_between(here, here)
    choices = [[(h, None, 0)] + [(v, when, 1) for v, when in moves(a)] for a, h in zip(AXES, here)]
    routes = []
    for x, when_x, far_x in choices[0]:
        for y, when_y, far_y in choices[1]:
            for z, when_z, far_z in choices[2]:
                if far_x + far_y + far_z:
                    routes.append((far_x + far_y, far_z, (x, y, z), both(when_x, when_y, when_z)))
    routes.sort(key=lambda r: (r[0] > 0, r[0]))

    def device(there):
        return dict(zip(AXES, there))

    barrier = pltpu.get_barrier_semaphore()

    def hello(there):
        pl.semaphore_signal(barrier, inc=1, device_id=device(there), device_id_type=MESH)

    for _, _, there, when in routes:
        guarded(when, functools.partial(hello, there))

    for n in (1, 5, 2, 6):
        loads[n].wait()
    latent = latents_ref[0, 0, 0]
    place = offsets_ref[0, 0, 0].astype(f32)
    rel = w_rel[0].astype(f32)
    rows = lax.broadcasted_iota(jnp.int32, (PACK, slots), 0)
    extra = jnp.zeros((PACK, slots), f32)
    for c in range(3):
        extra = jnp.where(rows == c, place[c : c + 1, :], extra)
        extra = jnp.where(rows == 3 + c, here[c].astype(f32), extra)
    col_ids = lax.broadcasted_iota(jnp.int32, (slots, slots), 0)
    spread = jnp.zeros((slots, slots), f32)
    rel_rows = jnp.zeros((slots, width), f32)
    for c in range(3):
        spread = jnp.where(col_ids == c, place[c : c + 1, :], spread)
        rel_rows = jnp.where(col_ids == c, rel[c : c + 1, :], rel_rows)
    rel_rows = rel_rows.astype(bf16)
    shift = dot(jnp.transpose(spread).astype(bf16), rel_rows)
    table[own, :slots, :] = (dot(latent, w_send[0]) + shift).astype(bf16)
    table[own, slots:, :] = extra.astype(bf16)

    peers = jnp.int32(0)
    for _, _, _, when in routes:
        peers = peers + (1 if when is None else when.astype(jnp.int32))
    pl.semaphore_wait(barrier, peers)

    sends = []
    for n, (_, far_z, there, when) in enumerate(routes):
        mine = slot_between(there, here)
        copy, arrival = [
            pltpu.make_async_remote_copy(
                src_ref=table.at[own], dst_ref=table.at[spot], send_sem=send_sem.at[n],
                recv_sem=recv_sem.at[spot], device_id=device(there), device_id_type=MESH,
            )
            for spot in (slot_between(here, there), mine)
        ]
        sends.append((when, copy, arrival, mine))
    for when, copy, _, _ in sends:
        guarded(when, copy.start)

    def clear(which):
        table[which] = jnp.zeros(table.shape[1:], bf16)

    for when, _, _, mine in sends:
        if when is not None:
            pl.when(jnp.logical_not(when))(functools.partial(clear, mine))

    for n in (3, 0, 4, 7, 8, 9):
        loads[n].wait()
    ids = jnp.concatenate([neighbours_ref[0, 0][:, b * slots : (b + 1) * slots] for b in range(blocks)], axis=0)
    cell, at = split(ids, slots)
    cell, z = split(cell, sizes[2])
    x, y = split(cell, sizes[1])
    found = [v - h + 1 if wide(a) else v for a, v, h in zip(AXES, (x, y, z), here)]
    spot = slot(found)
    index = lax.broadcasted_iota(jnp.int32, (blocks, slots), 0) * slots
    index = index + lax.broadcasted_iota(jnp.int32, (blocks, slots), 1)
    live = index < counts_ref[0]
    own_line = own // span_z
    near_by = jnp.logical_and(spot >= own_line * span_z, spot < (own_line + 1) * span_z)
    early = jnp.where(jnp.logical_and(live, near_by), 1.0, 0.0)
    late = jnp.where(live, 1.0, 0.0) - early
    marks = jnp.concatenate([early, late, jnp.zeros((PACK - 2 * blocks, slots), f32)], axis=0).astype(bf16)
    a = lax.broadcasted_iota(jnp.int32, (slots, slots), 0)
    b = lax.broadcasted_iota(jnp.int32, (slots, slots), 1)
    ahead = jnp.concatenate([jnp.where(a < b, 1.0, 0.0), jnp.ones((slots, slots), f32)], axis=1).astype(bf16)
    ranks = dot(marks, ahead)
    rank, whole = ranks[:, :slots], ranks[:, slots:]
    n_early = sum(whole[b : b + 1] for b in range(blocks))
    n_late = sum(whole[blocks + b : blocks + b + 1] for b in range(blocks))
    start = jnp.maximum(n_early, float(slots))
    tally[...] = jnp.broadcast_to(start + n_late - float(slots), tally.shape)
    order = lax.broadcasted_iota(jnp.int32, (room, slots), 0).astype(f32)
    picks, high, low = [], [], []
    base_early, base_late = jnp.zeros((1, slots), f32), start
    for b in range(blocks):
        first = jnp.where(early[b : b + 1] > 0, rank[b : b + 1] + base_early, -1.0)
        goal = jnp.where(late[b : b + 1] > 0, rank[blocks + b : blocks + b + 1] + base_late, first)
        base_early = base_early + whole[b : b + 1]
        base_late = base_late + whole[blocks + b : blocks + b + 1]
        picks.append(jnp.where(order == goal, 1.0, 0.0).astype(bf16))
        high.append((spot[b : b + 1] * slots).astype(f32))
        low.append((at[b : b + 1] + 1).astype(f32))
    picks = jnp.concatenate(picks, axis=1)
    high = jnp.broadcast_to(jnp.concatenate(high, axis=1), (slots, senders)).astype(bf16)
    low = jnp.broadcast_to(jnp.concatenate(low, axis=1), (slots, senders)).astype(bf16)
    sorted_ids = dot_nt(picks, high) + dot_nt(picks, low)
    masked[...] = jnp.where(sorted_ids > 0.5, 0.5 * b_edge[...], -1e30).astype(bf16)
    sorted_ids = sorted_ids.astype(jnp.int32) - 1
    lanes = lax.broadcasted_iota(jnp.int32, (room, slots), 1)

    cell_x, cell_z = split(a, spans[2])
    cell_x, cell_y = split(cell_x, spans[1])
    step = jnp.zeros((slots, width), f32)
    for c, v in enumerate((cell_x, cell_y, cell_z)):
        gap = v - 1 if wide(AXES[c]) else v - here[c]
        step = step + gap.astype(f32) * rel[c : c + 1]
    step_high = step.astype(bf16)
    step_low = (step - step_high.astype(f32)).astype(bf16)
    of_cell = jnp.where(lax.shift_right_arithmetic(sorted_ids, slots.bit_length() - 1) == lanes, 1.0, 0.0).astype(bf16)
    moved = dot(of_cell, step_high) + dot(of_cell, step_low)

    def choose(line):
        for k in range(span_z):
            hit = sorted_ids - (line * span_z + k) * slots == lanes
            chosen[line, :, k * slots : (k + 1) * slots] = jnp.where(hit, 1.0, 0.0).astype(bf16)

    for line in range(count // span_z):
        choose(line)

    edge_half = 0.5 * w_edge[0].astype(f32)
    nil = jnp.zeros_like(edge_half)
    pair_edge[...] = jnp.concatenate(
        [jnp.concatenate([edge_half, nil], axis=1), jnp.concatenate([nil, edge_half], axis=1)], axis=0
    ).astype(bf16)
    rel_half = (0.5 * rel[3:4]).astype(bf16)
    recv_half[...] = 0.5 * (dot(latent, w_recv[0]) + b_first[...] - shift)
    place_cols = [jnp.transpose(jnp.broadcast_to(place[c : c + 1], (slots, slots))) for c in range(3)]

    def gather(line, top, bottom):
        picked, cells = chosen[line, top:bottom, :], table.at[pl.ds(line * span_z, span_z)]
        rows_of = cells[:, :slots, :].reshape(span_z * slots, width)
        extras = cells[:, slots:, :]
        extras = jnp.concatenate([extras[k] for k in range(span_z)], axis=1)
        return dot(picked, rows_of), dot_nt(extras, picked)

    def place_block(b, feats):
        square = jnp.zeros((slots, slots), f32)
        for c in range(3):
            where = feats[c : c + 1] + (feats[3 + c : 4 + c] - here[c].astype(f32))
            apart = where - place_cols[c]
            square = square + apart * apart
        near[b] = 0.25 * square

    for (far, far_z, _, when), (_, _, arrival, _) in zip(routes, sends):
        if far == 0:
            guarded(when, arrival.wait_recv)
    rows_of, feats = gather(own_line, 0, room)
    send_half[:slots, :] = (0.5 * (rows_of[:slots] + moved[:slots])).astype(bf16)
    place_block(0, feats[:, :slots])
    carry = (rows_of[slots:] + moved[slots:], feats[:, slots:])

    @pl.loop(0, slots // EARLY_GROUP)
    def _(group):
        base = pl.multiple_of(group * EARLY_GROUP, EARLY_GROUP)
        own_rows = recv_half[pl.ds(base, EARLY_GROUP), :].astype(bf16)
        near_rows = near[0, pl.ds(base, EARLY_GROUP), :].astype(bf16)
        for i in range(0, EARLY_GROUP, 2):
            edges = edges_of(own_rows[i : i + 2], near_rows[i : i + 2], send_half[:slots, :], rel_half)
            sums = messages_of(dot(edges, pair_edge[...]), masked[:slots, :])
            for n in range(2):
                part[pl.ds(pl.multiple_of((base + i + n) * 8, 8), 8), :] = sums[n]

    pooled[...] = fold_rows(part, slots)

    pairs = {}
    for (far, far_z, there, when), (_, _, arrival, mine) in zip(routes, sends):
        if far:
            guarded(when, arrival.wait_recv)
            pairs.setdefault((id(there[0]), id(there[1])), []).append(mine)
            if len(pairs[id(there[0]), id(there[1])]) == span_z:
                rows_of, feats = gather(mine // span_z, slots, room)
                carry = (carry[0] + rows_of, carry[1] + feats)
    send_half[slots:, :] = (0.5 * carry[0]).astype(bf16)
    for b in range(blocks):
        place_block(b + 1, carry[1][:, b * slots : (b + 1) * slots])

    for when, copy, _, _ in sends:
        guarded(when, copy.wait_send)


B_LOADS = 6


def finish(*refs):
    send_half, near, recv_half, masked, pair_edge, pooled, tally = refs[:7]
    hbm, out_ref = refs[7 : 7 + B_LOADS], refs[7 + B_LOADS]
    held = refs[8 + B_LOADS : 8 + 2 * B_LOADS]
    load_sem, part = refs[8 + 2 * B_LOADS :]
    latents_ref, w_rel, w_self, w_agg, w_out, norm_gain = held
    loads = [pltpu.make_async_copy(src, dst, load_sem.at[n]) for n, (src, dst) in enumerate(zip(hbm, held))]
    for n in (1, 0, 2, 3, 4, 5):
        loads[n].start()
    slots, width = recv_half.shape
    used = jnp.max(tally[...]).astype(jnp.int32)
    steps = lax.div(used + (slots - 1), jnp.int32(slots)) * (slots // GROUP)
    part[...] = jnp.zeros_like(part)
    loads[1].wait()
    rel_half = (0.5 * w_rel[0][3:4].astype(f32)).astype(bf16)

    @pl.loop(0, steps)
    def _(step):
        block, group = split(step, slots // GROUP)
        block = block + 1
        top = pl.multiple_of(block * slots, slots)
        base = pl.multiple_of(group * GROUP, GROUP)
        own_rows = recv_half[pl.ds(base, GROUP), :].astype(bf16)
        near_rows = near[block, pl.ds(base, GROUP), :].astype(bf16)
        for i in range(0, GROUP, 2):
            edges = edges_of(own_rows[i : i + 2], near_rows[i : i + 2], send_half[pl.ds(top, slots), :], rel_half)
            sums = messages_of(dot(edges, pair_edge[...]), masked[pl.ds(top, slots), :])
            for n in range(2):
                spot = pl.ds(pl.multiple_of((base + i + n) * 8, 8), 8)
                part[spot, :] = part[spot, :] + sums[n]

    for n in (0, 2, 3, 4, 5):
        loads[n].wait()
    latent = latents_ref[0, 0, 0]
    mean = ((pooled[...] + fold_rows(part, slots)) / slots).astype(bf16)
    hidden = jax.nn.silu(dot(latent, w_self[0]) + dot(mean, w_agg[0])).astype(bf16)
    result = dot(hidden, w_out[0])
    center = jnp.mean(result, axis=-1, keepdims=True)
    shifted = result - center
    spread = jnp.mean(shifted * shifted, axis=-1, keepdims=True)
    normed = shifted * lax.rsqrt(spread + 1e-05) * norm_gain[...]
    out_ref[0, 0, 0] = (latent.astype(f32) + normed).astype(bf16)


def pinned(value):
    return pltpu.with_memory_space_constraint(value, pltpu.HBM)


def shards(
    latents, offsets, neighbours, counts, w_recv, w_send, w_rel, b_first, w_edge, b_edge, w_self, w_agg, w_out, norm_gain
):
    slots, width = latents.shape[3:]
    senders = neighbours.shape[3]
    room = senders + slots
    spans = [slots_of(axis) for axis in AXES]
    count = spans[0] * spans[1] * spans[2]
    vmem = pl.BlockSpec(memory_space=pltpu.VMEM)
    far = pl.BlockSpec(memory_space=pltpu.HBM)
    args = (counts, latents, offsets, neighbours, w_recv, w_send, w_rel, b_first, w_edge, b_edge)
    between = (
        ((room, width), bf16), ((room // slots, slots, slots), f32), ((slots, width), f32), ((room, width), bf16),
        ((2 * width, 2 * width), bf16), ((slots, width), f32), ((8, slots), f32),
    )
    found = pl.pallas_call(
        exchange,
        out_shape=[jax.ShapeDtypeStruct(*s) for s in between],
        in_specs=[far] * A_INPUTS,
        out_specs=[vmem] * A_OUTPUTS,
        scratch_shapes=[pltpu.VMEM(v.shape, v.dtype) for v in args]
        + [
            pltpu.SemaphoreType.DMA((A_INPUTS,)),
            pltpu.VMEM((count, slots + PACK, width), bf16),
            pltpu.VMEM((count // spans[2], room, slots * spans[2]), bf16),
            pltpu.VMEM((slots * 8, width), f32),
            pltpu.SemaphoreType.DMA((27,)),
            pltpu.SemaphoreType.DMA((count,)),
        ],
        compiler_params=pltpu.CompilerParams(
            collective_id=0, has_side_effects=True, vmem_limit_bytes=24 * 1024 * 1024
        ),
    )(args[0], *[pinned(v) for v in args[1:]])
    rest = tuple(pinned(v) for v in (latents, w_rel, w_self, w_agg, w_out, norm_gain))
    return pl.pallas_call(
        finish,
        out_shape=jax.ShapeDtypeStruct(latents.shape, latents.dtype),
        in_specs=[vmem] * A_OUTPUTS + [far] * B_LOADS,
        out_specs=vmem,
        scratch_shapes=[pltpu.VMEM(v.shape, v.dtype) for v in rest]
        + [pltpu.SemaphoreType.DMA((B_LOADS,)), pltpu.VMEM((slots * 8, width), f32)],
        compiler_params=pltpu.CompilerParams(vmem_limit_bytes=24 * 1024 * 1024),
    )(*found, *rest)


def solution(mesh):
    cells = ("groups", "gx"), "gy", "gz"
    in_specs = (P(*cells, None, None), P(*cells, None, None), P(*cells, None), P(*cells))
    in_specs += (P(),) * 10
    return jax.shard_map(
        shards, mesh=mesh, in_specs=in_specs, out_specs=P(*cells, None, None), check_vma=False
    )
```

```python
import functools

import jax
import jax.numpy as jnp
from jax import lax
from jax.experimental import pallas as pl
from jax.experimental.pallas import tpu as pltpu
from jax.sharding import PartitionSpec as P

MESH = pl.DeviceIdType.MESH
AXES = ("gx", "gy", "gz")
PACK = 16
GROUP = 64
CLASSES = 3
RELAYED = 2
NT = (((1,), (1,)), ((), ()))
f32, bf16 = jnp.float32, jnp.bfloat16


def split(value, size):
    if size & (size - 1) == 0:
        return value >> (size.bit_length() - 1), value & (size - 1)
    return lax.div(value, size), lax.rem(value, size)


def wide(axis):
    return lax.axis_size(axis) > 2


def slots_of(axis):
    return min(lax.axis_size(axis), 3)


def moves(axis):
    size, here = lax.axis_size(axis), lax.axis_index(axis)
    if size == 1:
        return []
    if size == 2:
        return [(1 - here, None)]
    return [(here - 1, here > 0), (here + 1, here < size - 1)]


def slot_on(axis, source, target):
    return source - target + 1 if wide(axis) else source


def both(*conditions):
    held = [c for c in conditions if c is not None]
    return functools.reduce(jnp.logical_and, held) if held else None


def guarded(condition, action):
    if condition is None:
        action()
    else:
        pl.when(condition)(action)


def dot(a, b):
    return jnp.dot(a, b, preferred_element_type=f32)


def dot_nt(a, b):
    return lax.dot_general(a, b, NT, preferred_element_type=f32)


def edges_of(own, near, send, rel_half):
    halves = []
    for n in range(2):
        gap = jnp.transpose(jnp.broadcast_to(near[n : n + 1], (send.shape[1], send.shape[0])))
        pre = (own[n : n + 1] + send) + gap * rel_half
        halves.append(pre * (jnp.tanh(pre) + 1))
    return jnp.concatenate(halves, axis=1)


def messages_of(result, masked):
    width = masked.shape[1]
    half, sums = result.astype(bf16), []
    for n in range(2):
        total = None
        for r in range(0, masked.shape[0], PACK):
            msg = half[r : r + PACK, n * width : (n + 1) * width] + masked[r : r + PACK]
            gate = jnp.tanh(msg) + 1
            term = msg.astype(f32) * gate.astype(f32)
            total = term if total is None else total + term
        sums.append(total[:8] + total[8:])
    return sums


def fold_rows(part, rows):
    total = part[pl.ds(0, rows, stride=8), :]
    for k in range(1, 8):
        total = total + part[pl.ds(k, rows, stride=8), :]
    return total


A_INPUTS = 10
A_OUTPUTS = 7
LOAD_ORDER = (1, 5, 2, 6, 3, 0, 4, 7, 8, 9)


def exchange(*refs):
    hbm, outs = refs[:A_INPUTS], refs[A_INPUTS : A_INPUTS + A_OUTPUTS]
    held = refs[A_INPUTS + A_OUTPUTS : 2 * A_INPUTS + A_OUTPUTS]
    load_sem, table, chosen, part, send_sem, relay_sem, recv_sem = refs[2 * A_INPUTS + A_OUTPUTS :]
    counts_ref, latents_ref, offsets_ref, neighbours_ref, w_recv, w_send, w_rel, b_first, w_edge, b_edge = held
    send_half, near, recv_half, masked, pair_edge, pooled, tally = outs
    loads = [pltpu.make_async_copy(src, dst, load_sem.at[n]) for n, (src, dst) in enumerate(zip(hbm, held))]
    for n in LOAD_ORDER:
        loads[n].start()
    slots, width = latents_ref.shape[3], latents_ref.shape[4]
    senders = neighbours_ref.shape[3]
    blocks, room = senders // slots, senders + (CLASSES - 1) * slots
    here = [lax.axis_index(axis) for axis in AXES]
    sizes = [lax.axis_size(axis) for axis in AXES]
    spans = [slots_of(axis) for axis in AXES]
    count, span_z = table.shape[0], spans[2]

    def slot(coords):
        return (coords[0] * spans[1] + coords[1]) * spans[2] + coords[2]

    def slot_between(source, target):
        return slot([slot_on(a, s, t) for a, s, t in zip(AXES, source, target)])

    own = slot_between(here, here)
    own_line = own // span_z
    choices = [[(h, None, 0)] + [(v, when, 1) for v, when in moves(a)] for a, h in zip(AXES[:2], here)]
    routes = []
    for x, when_x, far_x in choices[0]:
        for y, when_y, far_y in choices[1]:
            if far_x + far_y:
                routes.append((far_x + far_y, (x, y, here[2]), both(when_x, when_y)))
    routes.sort(key=lambda r: r[0])
    has_mate = sizes[2] > 1
    mate = (here[0], here[1], 1 - here[2])

    def device(there):
        return dict(zip(AXES, there))

    barrier = pltpu.get_barrier_semaphore()

    def hello(there):
        pl.semaphore_signal(barrier, inc=1, device_id=device(there), device_id_type=MESH)

    if has_mate:
        hello(mate)
    for far, there, when in routes:
        guarded(when, functools.partial(hello, there))
        if has_mate and far < RELAYED:
            guarded(when, functools.partial(hello, (there[0], there[1], mate[2])))

    for n in (1, 5, 2, 6):
        loads[n].wait()
    latent = latents_ref[0, 0, 0]
    place = offsets_ref[0, 0, 0].astype(f32)
    rel = w_rel[0].astype(f32)
    rows = lax.broadcasted_iota(jnp.int32, (PACK, slots), 0)
    extra = jnp.zeros((PACK, slots), f32)
    for c in range(3):
        extra = jnp.where(rows == c, place[c : c + 1, :], extra)
        extra = jnp.where(rows == 3 + c, here[c].astype(f32), extra)
    col_ids = lax.broadcasted_iota(jnp.int32, (slots, slots), 0)
    spread = jnp.zeros((slots, slots), f32)
    rel_rows = jnp.zeros((slots, width), f32)
    for c in range(3):
        spread = jnp.where(col_ids == c, place[c : c + 1, :], spread)
        rel_rows = jnp.where(col_ids == c, rel[c : c + 1, :], rel_rows)
    rel_rows = rel_rows.astype(bf16)
    shift = dot(jnp.transpose(spread).astype(bf16), rel_rows)
    table[own, :slots, :] = (dot(latent, w_send[0]) + shift).astype(bf16)
    table[own, slots:, :] = extra.astype(bf16)

    for n in (3, 0):
        loads[n].wait()
    ids = jnp.concatenate([neighbours_ref[0, 0][:, b * slots : (b + 1) * slots] for b in range(blocks)], axis=0)
    cell, at = split(ids, slots)
    cell, z = split(cell, sizes[2])
    x, y = split(cell, sizes[1])
    found = [v - h + 1 if wide(a) else v for a, v, h in zip(AXES, (x, y, z), here)]
    spot = slot(found)
    index = lax.broadcasted_iota(jnp.int32, (blocks, slots), 0) * slots
    index = index + lax.broadcasted_iota(jnp.int32, (blocks, slots), 1)
    live = index < counts_ref[0]
    apart = sum(jnp.where(found[c] == slot_on(AXES[c], here[c], here[c]), 0, 1) for c in range(2))
    classes = [jnp.where(jnp.logical_and(live, apart == k), 1.0, 0.0) for k in range(CLASSES)]
    spare = -(CLASSES * blocks) % PACK
    marks = jnp.concatenate(classes + [jnp.zeros((spare, slots), f32)], axis=0).astype(bf16)
    a = lax.broadcasted_iota(jnp.int32, (slots, slots), 0)
    b = lax.broadcasted_iota(jnp.int32, (slots, slots), 1)
    ahead = jnp.concatenate([jnp.where(a < b, 1.0, 0.0), jnp.ones((slots, slots), f32)], axis=1).astype(bf16)
    ranks = dot(marks, ahead)
    goals = [jnp.full((1, slots), -1.0, f32)] * blocks
    base = jnp.zeros((1, slots), f32)
    for k in range(CLASSES):
        base = jnp.maximum(base, float(k * slots))
        for b in range(blocks):
            row = slice(k * blocks + b, k * blocks + b + 1)
            goals[b] = jnp.where(classes[k][b : b + 1] > 0, ranks[row, :slots] + base, goals[b])
            base = base + ranks[row, slots:]
    tally[:8, :] = jnp.broadcast_to(base - float((CLASSES - 1) * slots), (8, slots))
    tally[8:, :] = jnp.broadcast_to(0.5 * rel[3:4], (8, width))

    peers = jnp.int32(1 if has_mate else 0)
    for far, _, when in routes:
        cores = 2 if has_mate and far < RELAYED else 1
        peers = peers + (cores if when is None else cores * when.astype(jnp.int32))
    pl.semaphore_wait(barrier, peers)

    def remote(source, spot, sem, there):
        return pltpu.make_async_remote_copy(
            src_ref=table.at[source], dst_ref=table.at[spot], send_sem=sem, recv_sem=recv_sem.at[spot],
            device_id=device(there), device_id_type=MESH,
        )

    lines, sends, relays = [(own_line, 0)], [], []
    for far, there, when in routes:
        mine = slot_between(there, here)
        twin = slot_between((there[0], there[1], mate[2]), here)
        lines.append((mine // span_z, far))
        other = (there[0], there[1], mate[2])
        n = len(sends)
        sends.append((far, when, remote(own, slot_between(here, there), send_sem.at[n], there),
                      remote(own, mine, send_sem.at[n], there), mine))
        if not has_mate:
            continue
        if far < RELAYED:
            sends.append((far, when, remote(own, slot_between(here, other), send_sem.at[n + 1], other),
                          remote(own, twin, send_sem.at[n + 1], other), twin))
        else:
            n = len(relays)
            relays.append((far, when, remote(mine, mine, relay_sem.at[n], mate), sends[-1][3],
                           remote(own, twin, relay_sem.at[n], mate), twin))
    if has_mate:
        mate_own = slot_between(mate, here)
        mate_copy = remote(own, own, send_sem.at[len(sends)], mate)
        mate_in = remote(own, mate_own, send_sem.at[len(sends)], mate)
        mate_copy.start()
    for _, when, copy, _, _ in sends:
        guarded(when, copy.start)

    def clear(which):
        table[which] = jnp.zeros(table.shape[1:], bf16)

    for when, which in [(s[1], s[4]) for s in sends] + [(r[1], r[5]) for r in relays]:
        if when is not None:
            pl.when(jnp.logical_not(when))(functools.partial(clear, which))

    for n in (4, 7, 8, 9):
        loads[n].wait()
    order = lax.broadcasted_iota(jnp.int32, (room, slots), 0).astype(f32)
    picks, high, low = [], [], []
    for b in range(blocks):
        picks.append(jnp.where(order == goals[b], 1.0, 0.0).astype(bf16))
        high.append((spot[b : b + 1] * slots).astype(f32))
        low.append((at[b : b + 1] + 1).astype(f32))
    picks = jnp.concatenate(picks, axis=1)
    high = jnp.broadcast_to(jnp.concatenate(high, axis=1), (slots, senders)).astype(bf16)
    low = jnp.broadcast_to(jnp.concatenate(low, axis=1), (slots, senders)).astype(bf16)
    sorted_ids = dot_nt(picks, high) + dot_nt(picks, low)
    masked[...] = jnp.where(sorted_ids > 0.5, 0.5 * b_edge[...], -1e30).astype(bf16)
    sorted_ids = sorted_ids.astype(jnp.int32) - 1
    lanes = lax.broadcasted_iota(jnp.int32, (room, slots), 1)

    cell_x, cell_z = split(lax.broadcasted_iota(jnp.int32, (slots, slots), 0), spans[2])
    cell_x, cell_y = split(cell_x, spans[1])
    step = jnp.zeros((slots, width), f32)
    for c, v in enumerate((cell_x, cell_y, cell_z)):
        gap = v - 1 if wide(AXES[c]) else v - here[c]
        step = step + gap.astype(f32) * rel[c : c + 1]
    step_high = step.astype(bf16)
    step_low = (step - step_high.astype(f32)).astype(bf16)
    of_cell = jnp.where(lax.shift_right_arithmetic(sorted_ids, slots.bit_length() - 1) == lanes, 1.0, 0.0).astype(bf16)
    moved = dot(of_cell, step_high) + dot(of_cell, step_low)

    for r, (line, far) in enumerate(lines):
        for k in range(span_z):
            hit = sorted_ids[far * slots :] - (line * span_z + k) * slots == lanes[far * slots :]
            chosen[r, far * slots :, k * slots : (k + 1) * slots] = jnp.where(hit, 1.0, 0.0).astype(bf16)

    edge_half = 0.5 * w_edge[0].astype(f32)
    nil = jnp.zeros_like(edge_half)
    pair_edge[...] = jnp.concatenate(
        [jnp.concatenate([edge_half, nil], axis=1), jnp.concatenate([nil, edge_half], axis=1)], axis=0
    ).astype(bf16)
    rel_half = (0.5 * rel[3:4]).astype(bf16)
    recv_half[...] = 0.5 * (dot(latent, w_recv[0]) + b_first[...] - shift)
    place_cols = [jnp.transpose(jnp.broadcast_to(place[c : c + 1], (slots, slots))) for c in range(3)]

    def gather(roles, top, bottom):
        total = moved[top:bottom], jnp.zeros((PACK, bottom - top), f32)
        for r in roles:
            picked, cells = chosen[r, top:bottom, :], table.at[pl.ds(lines[r][0] * span_z, span_z)]
            rows_of = cells[:, :slots, :].reshape(span_z * slots, width)
            extras = cells[:, slots:, :]
            extras = jnp.concatenate([extras[k] for k in range(span_z)], axis=1)
            total = total[0] + dot(picked, rows_of), total[1] + dot_nt(extras, picked)
        send_half[top:bottom, :] = (0.5 * total[0]).astype(bf16)
        for n in range(top // slots, bottom // slots):
            feats = total[1][:, n * slots - top : (n + 1) * slots - top]
            square = jnp.zeros((slots, slots), f32)
            for c in range(3):
                where = feats[c : c + 1] + (feats[3 + c : 4 + c] - here[c].astype(f32))
                gap = where - place_cols[c]
                square = square + gap * gap
            near[n] = 0.25 * square

    def pass_on():
        for _, when, relay, arrival, _, _ in relays:

            def forward(arrival=arrival, relay=relay):
                arrival.wait_recv()
                relay.start()

            guarded(when, forward)

    def work(block):
        top = block * slots

        @pl.loop(0, slots // GROUP)
        def _(group):
            base = pl.multiple_of(group * GROUP, GROUP)
            own_rows = recv_half[pl.ds(base, GROUP), :].astype(bf16)
            near_rows = near[block, pl.ds(base, GROUP), :].astype(bf16)
            for i in range(0, GROUP, 2):
                edges = edges_of(own_rows[i : i + 2], near_rows[i : i + 2], send_half[top : top + slots, :], rel_half)
                sums = messages_of(dot(edges, pair_edge[...]), masked[top : top + slots, :])
                for n in range(2):
                    eight = pl.ds(pl.multiple_of((base + i + n) * 8, 8), 8)
                    part[eight, :] = part[eight, :] + sums[n] if block else sums[n]

            if block + 1 == RELAYED:
                pl.when(group == 0)(pass_on)

    for far in range(CLASSES):
        if has_mate and far == 0:
            mate_in.wait_recv()
        for step_far, when, _, arrival, _ in sends:
            if step_far == far and not (has_mate and far >= RELAYED):
                guarded(when, arrival.wait_recv)
        for step_far, when, _, _, twin_in, _ in relays:
            if step_far == far:
                guarded(when, twin_in.wait_recv)
        roles = [r for r, (_, step_far) in enumerate(lines) if step_far <= far]
        gather(roles, far * slots, room if far == CLASSES - 1 else (far + 1) * slots)
        if far < CLASSES - 1:
            work(far)
        if far == CLASSES - 2:
            pooled[...] = fold_rows(part, slots)

    for when, copy in [(s[1], s[2]) for s in sends] + [(r[1], r[2]) for r in relays]:
        guarded(when, copy.wait_send)
    if has_mate:
        mate_copy.wait_send()


B_LOADS = 5


def finish(*refs):
    send_half, near, recv_half, masked, pair_edge, pooled, tally = refs[:7]
    hbm, out_ref = refs[7 : 7 + B_LOADS], refs[7 + B_LOADS]
    held = refs[8 + B_LOADS : 8 + 2 * B_LOADS]
    load_sem, part = refs[8 + 2 * B_LOADS :]
    latents_ref, w_self, w_agg, w_out, norm_gain = held
    loads = [pltpu.make_async_copy(src, dst, load_sem.at[n]) for n, (src, dst) in enumerate(zip(hbm, held))]
    for load in loads:
        load.start()
    slots, width = recv_half.shape
    used = jnp.max(tally[:8, :]).astype(jnp.int32)
    steps = lax.div(used + (slots - 1), jnp.int32(slots)) * (slots // GROUP)
    part[...] = jnp.zeros_like(part)
    rel_half = tally[8:9, :].astype(bf16)

    @pl.loop(0, steps)
    def _(step):
        block, group = split(step, slots // GROUP)
        block = block + (CLASSES - 1)
        top = pl.multiple_of(block * slots, slots)
        base = pl.multiple_of(group * GROUP, GROUP)
        own_rows = recv_half[pl.ds(base, GROUP), :].astype(bf16)
        near_rows = near[block, pl.ds(base, GROUP), :].astype(bf16)
        for i in range(0, GROUP, 2):
            edges = edges_of(own_rows[i : i + 2], near_rows[i : i + 2], send_half[pl.ds(top, slots), :], rel_half)
            sums = messages_of(dot(edges, pair_edge[...]), masked[pl.ds(top, slots), :])
            for n in range(2):
                spot = pl.ds(pl.multiple_of((base + i + n) * 8, 8), 8)
                part[spot, :] = part[spot, :] + sums[n]

    for load in loads:
        load.wait()
    latent = latents_ref[0, 0, 0]
    mean = ((pooled[...] + fold_rows(part, slots)) / slots).astype(bf16)
    hidden = jax.nn.silu(dot(latent, w_self[0]) + dot(mean, w_agg[0])).astype(bf16)
    result = dot(hidden, w_out[0])
    center = jnp.mean(result, axis=-1, keepdims=True)
    shifted = result - center
    spread = jnp.mean(shifted * shifted, axis=-1, keepdims=True)
    normed = shifted * lax.rsqrt(spread + 1e-05) * norm_gain[...]
    out_ref[0, 0, 0] = (latent.astype(f32) + normed).astype(bf16)


def pinned(value):
    return pltpu.with_memory_space_constraint(value, pltpu.HBM)


def shards(
    latents, offsets, neighbours, counts, w_recv, w_send, w_rel, b_first, w_edge, b_edge, w_self, w_agg, w_out, norm_gain
):
    slots, width = latents.shape[3:]
    senders = neighbours.shape[3]
    room = senders + (CLASSES - 1) * slots
    spans = [slots_of(axis) for axis in AXES]
    count = spans[0] * spans[1] * spans[2]
    vmem = pl.BlockSpec(memory_space=pltpu.VMEM)
    far = pl.BlockSpec(memory_space=pltpu.HBM)
    args = (counts, latents, offsets, neighbours, w_recv, w_send, w_rel, b_first, w_edge, b_edge)
    between = (
        ((room, width), bf16), ((room // slots, slots, slots), f32), ((slots, width), f32), ((room, width), bf16),
        ((2 * width, 2 * width), bf16), ((slots, width), f32), ((16, slots), f32),
    )
    found = pl.pallas_call(
        exchange,
        out_shape=[jax.ShapeDtypeStruct(*s) for s in between],
        in_specs=[far] * A_INPUTS,
        out_specs=[vmem] * A_OUTPUTS,
        scratch_shapes=[pltpu.VMEM(v.shape, v.dtype) for v in args]
        + [
            pltpu.SemaphoreType.DMA((A_INPUTS,)),
            pltpu.VMEM((count, slots + PACK, width), bf16),
            pltpu.VMEM((count // spans[2], room, slots * spans[2]), bf16),
            pltpu.VMEM((slots * 8, width), f32),
            pltpu.SemaphoreType.DMA((18,)),
            pltpu.SemaphoreType.DMA((9,)),
            pltpu.SemaphoreType.DMA((count,)),
        ],
        compiler_params=pltpu.CompilerParams(
            collective_id=0, has_side_effects=True, vmem_limit_bytes=24 * 1024 * 1024
        ),
    )(args[0], *[pinned(v) for v in args[1:]])
    rest = tuple(pinned(v) for v in (latents, w_self, w_agg, w_out, norm_gain))
    return pl.pallas_call(
        finish,
        out_shape=jax.ShapeDtypeStruct(latents.shape, latents.dtype),
        in_specs=[vmem] * A_OUTPUTS + [far] * B_LOADS,
        out_specs=vmem,
        scratch_shapes=[pltpu.VMEM(v.shape, v.dtype) for v in rest]
        + [pltpu.SemaphoreType.DMA((B_LOADS,)), pltpu.VMEM((slots * 8, width), f32)],
        compiler_params=pltpu.CompilerParams(vmem_limit_bytes=24 * 1024 * 1024),
    )(*found, *rest)


def solution(mesh):
    cells = ("groups", "gx"), "gy", "gz"
    in_specs = (P(*cells, None, None), P(*cells, None, None), P(*cells, None), P(*cells))
    in_specs += (P(),) * 10
    return jax.shard_map(
        shards, mesh=mesh, in_specs=in_specs, out_specs=P(*cells, None, None), check_vma=False
    )
```

```python
import functools

import jax
import jax.numpy as jnp
from jax import lax
from jax.experimental import pallas as pl
from jax.experimental.pallas import tpu as pltpu
from jax.sharding import PartitionSpec as P

MESH = pl.DeviceIdType.MESH
AXES = ("gx", "gy", "gz")
PACK = 16
GROUP = 64
CLASSES = 3
RELAYED = 2
NT = (((1,), (1,)), ((), ()))
f32, bf16 = jnp.float32, jnp.bfloat16


def split(value, size):
    if size & (size - 1) == 0:
        return value >> (size.bit_length() - 1), value & (size - 1)
    return lax.div(value, size), lax.rem(value, size)


def wide(axis):
    return lax.axis_size(axis) > 2


def slots_of(axis):
    return min(lax.axis_size(axis), 3)


def moves(axis):
    size, here = lax.axis_size(axis), lax.axis_index(axis)
    if size == 1:
        return []
    if size == 2:
        return [(1 - here, None)]
    return [(here - 1, here > 0), (here + 1, here < size - 1)]


def slot_on(axis, source, target):
    return source - target + 1 if wide(axis) else source


def both(*conditions):
    held = [c for c in conditions if c is not None]
    return functools.reduce(jnp.logical_and, held) if held else None


def guarded(condition, action):
    if condition is None:
        action()
    else:
        pl.when(condition)(action)


def dot(a, b):
    return jnp.dot(a, b, preferred_element_type=f32)


def dot_nt(a, b):
    return lax.dot_general(a, b, NT, preferred_element_type=f32)


def edges_of(own, near, send, rel_half):
    halves = []
    for n in range(2):
        gap = jnp.transpose(jnp.broadcast_to(near[n : n + 1], (send.shape[1], send.shape[0])))
        pre = (own[n : n + 1] + send) + gap * rel_half
        halves.append(pre * (jnp.tanh(pre) + 1))
    return jnp.concatenate(halves, axis=1)


def messages_of(result, masked):
    width = masked.shape[1]
    half, sums = result.astype(bf16), []
    for n in range(2):
        total = None
        for r in range(0, masked.shape[0], PACK):
            msg = half[r : r + PACK, n * width : (n + 1) * width] + masked[r : r + PACK]
            gate = jnp.tanh(msg) + 1
            term = msg.astype(f32) * gate.astype(f32)
            total = term if total is None else total + term
        sums.append(total[:8] + total[8:])
    return sums


def fold_rows(part, rows):
    total = part[pl.ds(0, rows, stride=8), :]
    for k in range(1, 8):
        total = total + part[pl.ds(k, rows, stride=8), :]
    return total


A_INPUTS = 10
A_OUTPUTS = 7
LOAD_ORDER = (1, 5, 2, 6, 3, 0, 4, 7, 8, 9)


def exchange(*refs):
    hbm, outs = refs[:A_INPUTS], refs[A_INPUTS : A_INPUTS + A_OUTPUTS]
    held = refs[A_INPUTS + A_OUTPUTS : 2 * A_INPUTS + A_OUTPUTS]
    load_sem, table, chosen, part, send_sem, relay_sem, recv_sem = refs[2 * A_INPUTS + A_OUTPUTS :]
    counts_ref, latents_ref, offsets_ref, neighbours_ref, w_recv, w_send, w_rel, b_first, w_edge, b_edge = held
    send_half, near, recv_half, masked, pair_edge, pooled, tally = outs
    loads = [pltpu.make_async_copy(src, dst, load_sem.at[n]) for n, (src, dst) in enumerate(zip(hbm, held))]
    for n in LOAD_ORDER:
        loads[n].start()
    slots, width = latents_ref.shape[3], latents_ref.shape[4]
    senders = neighbours_ref.shape[3]
    blocks, room = senders // slots, senders + (CLASSES - 1) * slots
    here = [lax.axis_index(axis) for axis in AXES]
    sizes = [lax.axis_size(axis) for axis in AXES]
    spans = [slots_of(axis) for axis in AXES]
    count, span_z = table.shape[0], spans[2]

    def slot(coords):
        return (coords[0] * spans[1] + coords[1]) * spans[2] + coords[2]

    def slot_between(source, target):
        return slot([slot_on(a, s, t) for a, s, t in zip(AXES, source, target)])

    own = slot_between(here, here)
    own_line = own // span_z
    choices = [[(h, None, 0)] + [(v, when, 1) for v, when in moves(a)] for a, h in zip(AXES[:2], here)]
    routes = []
    for x, when_x, far_x in choices[0]:
        for y, when_y, far_y in choices[1]:
            if far_x + far_y:
                routes.append((far_x + far_y, (x, y, here[2]), both(when_x, when_y)))
    routes.sort(key=lambda r: r[0])
    has_mate = sizes[2] > 1
    mate = (here[0], here[1], 1 - here[2])

    def device(there):
        return dict(zip(AXES, there))

    barrier = pltpu.get_barrier_semaphore()

    def hello(there):
        pl.semaphore_signal(barrier, inc=1, device_id=device(there), device_id_type=MESH)

    if has_mate:
        hello(mate)
    for far, there, when in routes:
        guarded(when, functools.partial(hello, there))
        if has_mate and far < RELAYED:
            guarded(when, functools.partial(hello, (there[0], there[1], mate[2])))

    for n in (1, 5, 2, 6):
        loads[n].wait()
    latent = latents_ref[0, 0, 0]
    place = offsets_ref[0, 0, 0].astype(f32)
    rel = w_rel[0].astype(f32)
    rows = lax.broadcasted_iota(jnp.int32, (PACK, slots), 0)
    extra = jnp.zeros((PACK, slots), f32)
    for c in range(3):
        extra = jnp.where(rows == c, place[c : c + 1, :], extra)
        extra = jnp.where(rows == 3 + c, here[c].astype(f32), extra)
    col_ids = lax.broadcasted_iota(jnp.int32, (slots, slots), 0)
    spread = jnp.zeros((slots, slots), f32)
    rel_rows = jnp.zeros((slots, width), f32)
    for c in range(3):
        spread = jnp.where(col_ids == c, place[c : c + 1, :], spread)
        rel_rows = jnp.where(col_ids == c, rel[c : c + 1, :], rel_rows)
    rel_rows = rel_rows.astype(bf16)
    shift = dot(jnp.transpose(spread).astype(bf16), rel_rows)
    table[own, :slots, :] = (dot(latent, w_send[0]) + shift).astype(bf16)
    table[own, slots:, :] = extra.astype(bf16)

    for n in (3, 0):
        loads[n].wait()
    ids = jnp.concatenate([neighbours_ref[0, 0][:, b * slots : (b + 1) * slots] for b in range(blocks)], axis=0)
    cell, at = split(ids, slots)
    cell, z = split(cell, sizes[2])
    x, y = split(cell, sizes[1])
    found = [v - h + 1 if wide(a) else v for a, v, h in zip(AXES, (x, y, z), here)]
    spot = slot(found)
    index = lax.broadcasted_iota(jnp.int32, (blocks, slots), 0) * slots
    index = index + lax.broadcasted_iota(jnp.int32, (blocks, slots), 1)
    live = index < counts_ref[0]
    apart = sum(jnp.where(found[c] == slot_on(AXES[c], here[c], here[c]), 0, 1) for c in range(2))
    classes = [jnp.where(jnp.logical_and(live, apart == k), 1.0, 0.0) for k in range(CLASSES)]
    spare = -(CLASSES * blocks) % PACK
    marks = jnp.concatenate(classes + [jnp.zeros((spare, slots), f32)], axis=0).astype(bf16)
    a = lax.broadcasted_iota(jnp.int32, (slots, slots), 0)
    b = lax.broadcasted_iota(jnp.int32, (slots, slots), 1)
    ahead = jnp.concatenate([jnp.where(a < b, 1.0, 0.0), jnp.ones((slots, slots), f32)], axis=1).astype(bf16)
    ranks = dot(marks, ahead)
    goals = [jnp.full((1, slots), -1.0, f32)] * blocks
    base = jnp.zeros((1, slots), f32)
    for k in range(CLASSES):
        base = jnp.maximum(base, float(k * slots))
        for b in range(blocks):
            row = slice(k * blocks + b, k * blocks + b + 1)
            goals[b] = jnp.where(classes[k][b : b + 1] > 0, ranks[row, :slots] + base, goals[b])
            base = base + ranks[row, slots:]
    tally[:8, :] = jnp.broadcast_to(base - float((CLASSES - 1) * slots), (8, slots))
    tally[8:, :] = jnp.broadcast_to(0.5 * rel[3:4], (8, width))

    for n in (4, 7, 8, 9):
        loads[n].wait()
    order = lax.broadcasted_iota(jnp.int32, (room, slots), 0).astype(f32)
    picks, high, low = [], [], []
    for b in range(blocks):
        picks.append(jnp.where(order == goals[b], 1.0, 0.0).astype(bf16))
        high.append((spot[b : b + 1] * slots).astype(f32))
        low.append((at[b : b + 1] + 1).astype(f32))
    picks = jnp.concatenate(picks, axis=1)
    high = jnp.broadcast_to(jnp.concatenate(high, axis=1), (slots, senders)).astype(bf16)
    low = jnp.broadcast_to(jnp.concatenate(low, axis=1), (slots, senders)).astype(bf16)
    sorted_ids = dot_nt(picks, high) + dot_nt(picks, low)
    masked[...] = jnp.where(sorted_ids > 0.5, 0.5 * b_edge[...], -1e30).astype(bf16)
    sorted_ids = sorted_ids.astype(jnp.int32) - 1
    lanes = lax.broadcasted_iota(jnp.int32, (room, slots), 1)

    cell_x, cell_z = split(lax.broadcasted_iota(jnp.int32, (slots, slots), 0), spans[2])
    cell_x, cell_y = split(cell_x, spans[1])
    step = jnp.zeros((slots, width), f32)
    for c, v in enumerate((cell_x, cell_y, cell_z)):
        gap = v - 1 if wide(AXES[c]) else v - here[c]
        step = step + gap.astype(f32) * rel[c : c + 1]
    step_high = step.astype(bf16)
    step_low = (step - step_high.astype(f32)).astype(bf16)
    of_cell = jnp.where(lax.shift_right_arithmetic(sorted_ids, slots.bit_length() - 1) == lanes, 1.0, 0.0).astype(bf16)
    moved = dot(of_cell, step_high) + dot(of_cell, step_low)

    peers = jnp.int32(1 if has_mate else 0)
    for far, _, when in routes:
        cores = 2 if has_mate and far < RELAYED else 1
        peers = peers + (cores if when is None else cores * when.astype(jnp.int32))
    pl.semaphore_wait(barrier, peers)

    def remote(source, spot, sem, there):
        return pltpu.make_async_remote_copy(
            src_ref=table.at[source], dst_ref=table.at[spot], send_sem=sem, recv_sem=recv_sem.at[spot],
            device_id=device(there), device_id_type=MESH,
        )

    lines, sends, relays = [(own_line, 0)], [], []
    for far, there, when in routes:
        mine = slot_between(there, here)
        twin = slot_between((there[0], there[1], mate[2]), here)
        lines.append((mine // span_z, far))
        other = (there[0], there[1], mate[2])
        n = len(sends)
        sends.append((far, when, remote(own, slot_between(here, there), send_sem.at[n], there),
                      remote(own, mine, send_sem.at[n], there), mine))
        if not has_mate:
            continue
        if far < RELAYED:
            sends.append((far, when, remote(own, slot_between(here, other), send_sem.at[n + 1], other),
                          remote(own, twin, send_sem.at[n + 1], other), twin))
        else:
            n = len(relays)
            relays.append((far, when, remote(mine, mine, relay_sem.at[n], mate), sends[-1][3],
                           remote(own, twin, relay_sem.at[n], mate), twin))
    if has_mate:
        mate_own = slot_between(mate, here)
        mate_copy = remote(own, own, send_sem.at[len(sends)], mate)
        mate_in = remote(own, mate_own, send_sem.at[len(sends)], mate)
        mate_copy.start()
    for _, when, copy, _, _ in sends:
        guarded(when, copy.start)

    def clear(which):
        table[which] = jnp.zeros(table.shape[1:], bf16)

    for when, which in [(s[1], s[4]) for s in sends] + [(r[1], r[5]) for r in relays]:
        if when is not None:
            pl.when(jnp.logical_not(when))(functools.partial(clear, which))

    for r, (line, far) in enumerate(lines):
        for k in range(span_z):
            hit = sorted_ids[far * slots :] - (line * span_z + k) * slots == lanes[far * slots :]
            chosen[r, far * slots :, k * slots : (k + 1) * slots] = jnp.where(hit, 1.0, 0.0).astype(bf16)

    edge_half = 0.5 * w_edge[0].astype(f32)
    nil = jnp.zeros_like(edge_half)
    pair_edge[...] = jnp.concatenate(
        [jnp.concatenate([edge_half, nil], axis=1), jnp.concatenate([nil, edge_half], axis=1)], axis=0
    ).astype(bf16)
    rel_half = (0.5 * rel[3:4]).astype(bf16)
    recv_half[...] = 0.5 * (dot(latent, w_recv[0]) + b_first[...] - shift)
    place_cols = [jnp.transpose(jnp.broadcast_to(place[c : c + 1], (slots, slots))) for c in range(3)]

    def gather(roles, top, bottom):
        total = moved[top:bottom], jnp.zeros((PACK, bottom - top), f32)
        for r in roles:
            picked, cells = chosen[r, top:bottom, :], table.at[pl.ds(lines[r][0] * span_z, span_z)]
            rows_of = cells[:, :slots, :].reshape(span_z * slots, width)
            extras = cells[:, slots:, :]
            extras = jnp.concatenate([extras[k] for k in range(span_z)], axis=1)
            total = total[0] + dot(picked, rows_of), total[1] + dot_nt(extras, picked)
        send_half[top:bottom, :] = (0.5 * total[0]).astype(bf16)
        for n in range(top // slots, bottom // slots):
            feats = total[1][:, n * slots - top : (n + 1) * slots - top]
            square = jnp.zeros((slots, slots), f32)
            for c in range(3):
                where = feats[c : c + 1] + (feats[3 + c : 4 + c] - here[c].astype(f32))
                gap = where - place_cols[c]
                square = square + gap * gap
            near[n] = 0.25 * square

    def pass_on():
        for _, when, relay, arrival, _, _ in relays:

            def forward(arrival=arrival, relay=relay):
                arrival.wait_recv()
                relay.start()

            guarded(when, forward)

    def work(block):
        top = block * slots

        @pl.loop(0, slots // GROUP)
        def _(group):
            base = pl.multiple_of(group * GROUP, GROUP)
            own_rows = recv_half[pl.ds(base, GROUP), :].astype(bf16)
            near_rows = near[block, pl.ds(base, GROUP), :].astype(bf16)
            for i in range(0, GROUP, 2):
                edges = edges_of(own_rows[i : i + 2], near_rows[i : i + 2], send_half[top : top + slots, :], rel_half)
                sums = messages_of(dot(edges, pair_edge[...]), masked[top : top + slots, :])
                for n in range(2):
                    eight = pl.ds(pl.multiple_of((base + i + n) * 8, 8), 8)
                    part[eight, :] = part[eight, :] + sums[n] if block else sums[n]

            if block + 1 == RELAYED:
                pl.when(group == 0)(pass_on)

    for far in range(CLASSES):
        if has_mate and far == 0:
            mate_in.wait_recv()
        for step_far, when, _, arrival, _ in sends:
            if step_far == far and not (has_mate and far >= RELAYED):
                guarded(when, arrival.wait_recv)
        for step_far, when, _, _, twin_in, _ in relays:
            if step_far == far:
                guarded(when, twin_in.wait_recv)
        roles = [r for r, (_, step_far) in enumerate(lines) if step_far <= far]
        gather(roles, far * slots, room if far == CLASSES - 1 else (far + 1) * slots)
        if far < CLASSES - 1:
            work(far)
        if far == CLASSES - 2:
            pooled[...] = fold_rows(part, slots)

    for when, copy in [(s[1], s[2]) for s in sends] + [(r[1], r[2]) for r in relays]:
        guarded(when, copy.wait_send)
    if has_mate:
        mate_copy.wait_send()


B_LOADS = 5


def finish(*refs):
    send_half, near, recv_half, masked, pair_edge, pooled, tally = refs[:7]
    hbm, out_ref = refs[7 : 7 + B_LOADS], refs[7 + B_LOADS]
    held = refs[8 + B_LOADS : 8 + 2 * B_LOADS]
    load_sem, part = refs[8 + 2 * B_LOADS :]
    latents_ref, w_self, w_agg, w_out, norm_gain = held
    loads = [pltpu.make_async_copy(src, dst, load_sem.at[n]) for n, (src, dst) in enumerate(zip(hbm, held))]
    for load in loads:
        load.start()
    slots, width = recv_half.shape
    used = jnp.max(tally[:8, :]).astype(jnp.int32)
    steps = lax.div(used + (slots - 1), jnp.int32(slots)) * (slots // GROUP)
    part[...] = jnp.zeros_like(part)
    rel_half = tally[8:9, :].astype(bf16)

    @pl.loop(0, steps)
    def _(step):
        block, group = split(step, slots // GROUP)
        block = block + (CLASSES - 1)
        top = pl.multiple_of(block * slots, slots)
        base = pl.multiple_of(group * GROUP, GROUP)
        own_rows = recv_half[pl.ds(base, GROUP), :].astype(bf16)
        near_rows = near[block, pl.ds(base, GROUP), :].astype(bf16)
        for i in range(0, GROUP, 2):
            edges = edges_of(own_rows[i : i + 2], near_rows[i : i + 2], send_half[pl.ds(top, slots), :], rel_half)
            sums = messages_of(dot(edges, pair_edge[...]), masked[pl.ds(top, slots), :])
            for n in range(2):
                spot = pl.ds(pl.multiple_of((base + i + n) * 8, 8), 8)
                part[spot, :] = part[spot, :] + sums[n]

    for load in loads:
        load.wait()
    latent = latents_ref[0, 0, 0]
    mean = ((pooled[...] + fold_rows(part, slots)) / slots).astype(bf16)
    hidden = jax.nn.silu(dot(latent, w_self[0]) + dot(mean, w_agg[0])).astype(bf16)
    result = dot(hidden, w_out[0])
    center = jnp.mean(result, axis=-1, keepdims=True)
    shifted = result - center
    spread = jnp.mean(shifted * shifted, axis=-1, keepdims=True)
    normed = shifted * lax.rsqrt(spread + 1e-05) * norm_gain[...]
    out_ref[0, 0, 0] = (latent.astype(f32) + normed).astype(bf16)


def pinned(value):
    return pltpu.with_memory_space_constraint(value, pltpu.HBM)


def shards(
    latents, offsets, neighbours, counts, w_recv, w_send, w_rel, b_first, w_edge, b_edge, w_self, w_agg, w_out, norm_gain
):
    slots, width = latents.shape[3:]
    senders = neighbours.shape[3]
    room = senders + (CLASSES - 1) * slots
    spans = [slots_of(axis) for axis in AXES]
    count = spans[0] * spans[1] * spans[2]
    vmem = pl.BlockSpec(memory_space=pltpu.VMEM)
    far = pl.BlockSpec(memory_space=pltpu.HBM)
    args = (counts, latents, offsets, neighbours, w_recv, w_send, w_rel, b_first, w_edge, b_edge)
    between = (
        ((room, width), bf16), ((room // slots, slots, slots), f32), ((slots, width), f32), ((room, width), bf16),
        ((2 * width, 2 * width), bf16), ((slots, width), f32), ((16, slots), f32),
    )
    found = pl.pallas_call(
        exchange,
        out_shape=[jax.ShapeDtypeStruct(*s) for s in between],
        in_specs=[far] * A_INPUTS,
        out_specs=[vmem] * A_OUTPUTS,
        scratch_shapes=[pltpu.VMEM(v.shape, v.dtype) for v in args]
        + [
            pltpu.SemaphoreType.DMA((A_INPUTS,)),
            pltpu.VMEM((count, slots + PACK, width), bf16),
            pltpu.VMEM((count // spans[2], room, slots * spans[2]), bf16),
            pltpu.VMEM((slots * 8, width), f32),
            pltpu.SemaphoreType.DMA((18,)),
            pltpu.SemaphoreType.DMA((9,)),
            pltpu.SemaphoreType.DMA((count,)),
        ],
        compiler_params=pltpu.CompilerParams(
            collective_id=0, has_side_effects=True, vmem_limit_bytes=24 * 1024 * 1024
        ),
    )(args[0], *[pinned(v) for v in args[1:]])
    rest = tuple(pinned(v) for v in (latents, w_self, w_agg, w_out, norm_gain))
    return pl.pallas_call(
        finish,
        out_shape=jax.ShapeDtypeStruct(latents.shape, latents.dtype),
        in_specs=[vmem] * A_OUTPUTS + [far] * B_LOADS,
        out_specs=vmem,
        scratch_shapes=[pltpu.VMEM(v.shape, v.dtype) for v in rest]
        + [pltpu.SemaphoreType.DMA((B_LOADS,)), pltpu.VMEM((slots * 8, width), f32)],
        compiler_params=pltpu.CompilerParams(vmem_limit_bytes=24 * 1024 * 1024),
    )(*found, *rest)


def solution(mesh):
    cells = ("groups", "gx"), "gy", "gz"
    in_specs = (P(*cells, None, None), P(*cells, None, None), P(*cells, None), P(*cells))
    in_specs += (P(),) * 10
    return jax.shard_map(
        shards, mesh=mesh, in_specs=in_specs, out_specs=P(*cells, None, None), check_vma=False
    )
```

```python
import functools

import jax
import jax.numpy as jnp
from jax import lax
from jax.experimental import pallas as pl
from jax.experimental.pallas import tpu as pltpu
from jax.sharding import PartitionSpec as P

MESH = pl.DeviceIdType.MESH
AXES = ("gx", "gy", "gz")
PACK = 16
GROUPS = (128, 64, 128)
CLASSES = 3
RELAYED = 2
NT = (((1,), (1,)), ((), ()))
f32, bf16 = jnp.float32, jnp.bfloat16


def split(value, size):
    if size & (size - 1) == 0:
        return value >> (size.bit_length() - 1), value & (size - 1)
    return lax.div(value, size), lax.rem(value, size)


def wide(axis):
    return lax.axis_size(axis) > 2


def slots_of(axis):
    return min(lax.axis_size(axis), 3)


def moves(axis):
    size, here = lax.axis_size(axis), lax.axis_index(axis)
    if size == 1:
        return []
    if size == 2:
        return [(1 - here, None)]
    return [(here - 1, here > 0), (here + 1, here < size - 1)]


def slot_on(axis, source, target):
    return source - target + 1 if wide(axis) else source


def both(*conditions):
    held = [c for c in conditions if c is not None]
    return functools.reduce(jnp.logical_and, held) if held else None


def guarded(condition, action):
    if condition is None:
        action()
    else:
        pl.when(condition)(action)


def dot(a, b):
    return jnp.dot(a, b, preferred_element_type=f32)


def dot_nt(a, b):
    return lax.dot_general(a, b, NT, preferred_element_type=f32)


def edges_of(own, near, send, rel_half):
    halves = []
    for n in range(2):
        gap = jnp.transpose(jnp.broadcast_to(near[n : n + 1], (send.shape[1], send.shape[0])))
        pre = (own[n : n + 1] + send) + gap * rel_half
        halves.append(pre * (jnp.tanh(pre) + 1))
    return jnp.concatenate(halves, axis=1)


def messages_of(result, masked):
    width = masked.shape[1]
    half, sums = result.astype(bf16), []
    for n in range(2):
        total = None
        for r in range(0, masked.shape[0], PACK):
            msg = half[r : r + PACK, n * width : (n + 1) * width] + masked[r : r + PACK]
            gate = jnp.tanh(msg) + 1
            term = msg.astype(f32) * gate.astype(f32)
            total = term if total is None else total + term
        sums.append(total[:8] + total[8:])
    return sums


def fold_rows(part, rows):
    total = part[pl.ds(0, rows, stride=8), :]
    for k in range(1, 8):
        total = total + part[pl.ds(k, rows, stride=8), :]
    return total


A_INPUTS = 10
A_OUTPUTS = 7
LOAD_ORDER = (1, 5, 2, 6, 3, 0, 4, 7, 8, 9)


def exchange(*refs):
    hbm, outs = refs[:A_INPUTS], refs[A_INPUTS : A_INPUTS + A_OUTPUTS]
    held = refs[A_INPUTS + A_OUTPUTS : 2 * A_INPUTS + A_OUTPUTS]
    load_sem, table, chosen, part, send_sem, relay_sem, recv_sem = refs[2 * A_INPUTS + A_OUTPUTS :]
    counts_ref, latents_ref, offsets_ref, neighbours_ref, w_recv, w_send, w_rel, b_first, w_edge, b_edge = held
    send_half, near, recv_half, masked, pair_edge, pooled, tally = outs
    loads = [pltpu.make_async_copy(src, dst, load_sem.at[n]) for n, (src, dst) in enumerate(zip(hbm, held))]
    for n in LOAD_ORDER:
        loads[n].start()
    slots, width = latents_ref.shape[3], latents_ref.shape[4]
    senders = neighbours_ref.shape[3]
    blocks, room = senders // slots, senders + (CLASSES - 1) * slots
    here = [lax.axis_index(axis) for axis in AXES]
    sizes = [lax.axis_size(axis) for axis in AXES]
    spans = [slots_of(axis) for axis in AXES]
    count, span_z = table.shape[0], spans[2]

    def slot(coords):
        return (coords[0] * spans[1] + coords[1]) * spans[2] + coords[2]

    def slot_between(source, target):
        return slot([slot_on(a, s, t) for a, s, t in zip(AXES, source, target)])

    own = slot_between(here, here)
    own_line = own // span_z
    choices = [[(h, None, 0)] + [(v, when, 1) for v, when in moves(a)] for a, h in zip(AXES[:2], here)]
    routes = []
    for x, when_x, far_x in choices[0]:
        for y, when_y, far_y in choices[1]:
            if far_x + far_y:
                routes.append((far_x + far_y, (x, y, here[2]), both(when_x, when_y)))
    routes.sort(key=lambda r: r[0])
    has_mate = sizes[2] > 1
    mate = (here[0], here[1], 1 - here[2])

    def device(there):
        return dict(zip(AXES, there))

    barrier = pltpu.get_barrier_semaphore()

    def hello(there):
        pl.semaphore_signal(barrier, inc=1, device_id=device(there), device_id_type=MESH)

    if has_mate:
        hello(mate)
    for far, there, when in routes:
        guarded(when, functools.partial(hello, there))
        if has_mate and far < RELAYED:
            guarded(when, functools.partial(hello, (there[0], there[1], mate[2])))

    for n in (1, 5, 2, 6):
        loads[n].wait()
    latent = latents_ref[0, 0, 0]
    place = offsets_ref[0, 0, 0].astype(f32)
    rel = w_rel[0].astype(f32)
    rows = lax.broadcasted_iota(jnp.int32, (PACK, slots), 0)
    extra = jnp.zeros((PACK, slots), f32)
    for c in range(3):
        extra = jnp.where(rows == c, place[c : c + 1, :], extra)
        extra = jnp.where(rows == 3 + c, here[c].astype(f32), extra)
    col_ids = lax.broadcasted_iota(jnp.int32, (slots, slots), 0)
    spread = jnp.zeros((slots, slots), f32)
    rel_rows = jnp.zeros((slots, width), f32)
    for c in range(3):
        spread = jnp.where(col_ids == c, place[c : c + 1, :], spread)
        rel_rows = jnp.where(col_ids == c, rel[c : c + 1, :], rel_rows)
    rel_rows = rel_rows.astype(bf16)
    shift = dot(jnp.transpose(spread).astype(bf16), rel_rows)
    table[own, :slots, :] = (dot(latent, w_send[0]) + shift).astype(bf16)
    table[own, slots:, :] = extra.astype(bf16)

    for n in (3, 0):
        loads[n].wait()
    ids = jnp.concatenate([neighbours_ref[0, 0][:, b * slots : (b + 1) * slots] for b in range(blocks)], axis=0)
    cell, at = split(ids, slots)
    cell, z = split(cell, sizes[2])
    x, y = split(cell, sizes[1])
    found = [v - h + 1 if wide(a) else v for a, v, h in zip(AXES, (x, y, z), here)]
    spot = slot(found)
    index = lax.broadcasted_iota(jnp.int32, (blocks, slots), 0) * slots
    index = index + lax.broadcasted_iota(jnp.int32, (blocks, slots), 1)
    live = index < counts_ref[0]
    apart = sum(jnp.where(found[c] == slot_on(AXES[c], here[c], here[c]), 0, 1) for c in range(2))
    classes = [jnp.where(jnp.logical_and(live, apart == k), 1.0, 0.0) for k in range(CLASSES)]
    spare = -(CLASSES * blocks) % PACK
    marks = jnp.concatenate(classes + [jnp.zeros((spare, slots), f32)], axis=0).astype(bf16)
    a = lax.broadcasted_iota(jnp.int32, (slots, slots), 0)
    b = lax.broadcasted_iota(jnp.int32, (slots, slots), 1)
    ahead = jnp.concatenate([jnp.where(a < b, 1.0, 0.0), jnp.ones((slots, slots), f32)], axis=1).astype(bf16)
    ranks = dot(marks, ahead)
    goals = [jnp.full((1, slots), -1.0, f32)] * blocks
    base = jnp.zeros((1, slots), f32)
    for k in range(CLASSES):
        base = jnp.maximum(base, float(k * slots))
        for b in range(blocks):
            row = slice(k * blocks + b, k * blocks + b + 1)
            goals[b] = jnp.where(classes[k][b : b + 1] > 0, ranks[row, :slots] + base, goals[b])
            base = base + ranks[row, slots:]
    tally[:8, :] = jnp.broadcast_to(base - float((CLASSES - 1) * slots), (8, slots))
    tally[8:, :] = jnp.broadcast_to(0.5 * rel[3:4], (8, width))

    for n in (4, 7, 8, 9):
        loads[n].wait()
    order = lax.broadcasted_iota(jnp.int32, (room, slots), 0).astype(f32)
    picks, high, low = [], [], []
    for b in range(blocks):
        picks.append(jnp.where(order == goals[b], 1.0, 0.0).astype(bf16))
        high.append((spot[b : b + 1] * slots).astype(f32))
        low.append((at[b : b + 1] + 1).astype(f32))
    picks = jnp.concatenate(picks, axis=1)
    high = jnp.broadcast_to(jnp.concatenate(high, axis=1), (slots, senders)).astype(bf16)
    low = jnp.broadcast_to(jnp.concatenate(low, axis=1), (slots, senders)).astype(bf16)
    sorted_ids = dot_nt(picks, high) + dot_nt(picks, low)
    masked[...] = jnp.where(sorted_ids > 0.5, 0.5 * b_edge[...], -1e30).astype(bf16)
    sorted_ids = sorted_ids.astype(jnp.int32) - 1
    lanes = lax.broadcasted_iota(jnp.int32, (room, slots), 1)

    cell_x, cell_z = split(lax.broadcasted_iota(jnp.int32, (slots, slots), 0), spans[2])
    cell_x, cell_y = split(cell_x, spans[1])
    step = jnp.zeros((slots, width), f32)
    for c, v in enumerate((cell_x, cell_y, cell_z)):
        gap = v - 1 if wide(AXES[c]) else v - here[c]
        step = step + gap.astype(f32) * rel[c : c + 1]
    step_high = step.astype(bf16)
    step_low = (step - step_high.astype(f32)).astype(bf16)
    of_cell = jnp.where(lax.shift_right_arithmetic(sorted_ids, slots.bit_length() - 1) == lanes, 1.0, 0.0).astype(bf16)
    moved = dot(of_cell, step_high) + dot(of_cell, step_low)

    peers = jnp.int32(1 if has_mate else 0)
    for far, _, when in routes:
        cores = 2 if has_mate and far < RELAYED else 1
        peers = peers + (cores if when is None else cores * when.astype(jnp.int32))
    pl.semaphore_wait(barrier, peers)

    def remote(source, spot, sem, there):
        return pltpu.make_async_remote_copy(
            src_ref=table.at[source], dst_ref=table.at[spot], send_sem=sem, recv_sem=recv_sem.at[spot],
            device_id=device(there), device_id_type=MESH,
        )

    lines, sends, relays = [(own_line, 0)], [], []
    for far, there, when in routes:
        mine = slot_between(there, here)
        twin = slot_between((there[0], there[1], mate[2]), here)
        lines.append((mine // span_z, far))
        other = (there[0], there[1], mate[2])
        n = len(sends)
        sends.append((far, when, remote(own, slot_between(here, there), send_sem.at[n], there),
                      remote(own, mine, send_sem.at[n], there), mine))
        if not has_mate:
            continue
        if far < RELAYED:
            sends.append((far, when, remote(own, slot_between(here, other), send_sem.at[n + 1], other),
                          remote(own, twin, send_sem.at[n + 1], other), twin))
        else:
            n = len(relays)
            relays.append((far, when, remote(mine, mine, relay_sem.at[n], mate), sends[-1][3],
                           remote(own, twin, relay_sem.at[n], mate), twin))
    if has_mate:
        mate_own = slot_between(mate, here)
        mate_copy = remote(own, own, send_sem.at[len(sends)], mate)
        mate_in = remote(own, mate_own, send_sem.at[len(sends)], mate)
        mate_copy.start()
    for _, when, copy, _, _ in sends:
        guarded(when, copy.start)

    def clear(which):
        table[which] = jnp.zeros(table.shape[1:], bf16)

    for when, which in [(s[1], s[4]) for s in sends] + [(r[1], r[5]) for r in relays]:
        if when is not None:
            pl.when(jnp.logical_not(when))(functools.partial(clear, which))

    for r, (line, far) in enumerate(lines):
        for k in range(span_z):
            hit = sorted_ids[far * slots :] - (line * span_z + k) * slots == lanes[far * slots :]
            chosen[r, far * slots :, k * slots : (k + 1) * slots] = jnp.where(hit, 1.0, 0.0).astype(bf16)

    edge_half = 0.5 * w_edge[0].astype(f32)
    nil = jnp.zeros_like(edge_half)
    pair_edge[...] = jnp.concatenate(
        [jnp.concatenate([edge_half, nil], axis=1), jnp.concatenate([nil, edge_half], axis=1)], axis=0
    ).astype(bf16)
    rel_half = (0.5 * rel[3:4]).astype(bf16)
    recv_half[...] = 0.5 * (dot(latent, w_recv[0]) + b_first[...] - shift)
    place_cols = [jnp.transpose(jnp.broadcast_to(place[c : c + 1], (slots, slots))) for c in range(3)]

    def gather(roles, top, bottom):
        total = jnp.concatenate([moved[top:bottom], jnp.zeros((bottom - top, PACK), f32)], axis=1)
        for r in roles:
            picked, cells = chosen[r, top:bottom, :], table.at[pl.ds(lines[r][0] * span_z, span_z)]
            sides = [jnp.transpose(cells[k, slots:, :].astype(f32)).astype(bf16) for k in range(span_z)]
            both_of = jnp.concatenate(
                [cells[:, :slots, :].reshape(span_z * slots, width), jnp.concatenate(sides, axis=0)], axis=1
            )
            total = total + dot(picked, both_of)
        send_half[top:bottom, :] = (0.5 * total[:, :width]).astype(bf16)
        for n in range(top // slots, bottom // slots):
            feats = jnp.transpose(total[n * slots - top : (n + 1) * slots - top, width:])
            square = jnp.zeros((slots, slots), f32)
            for c in range(3):
                where = feats[c : c + 1] + (feats[3 + c : 4 + c] - here[c].astype(f32))
                gap = where - place_cols[c]
                square = square + gap * gap
            near[n] = 0.25 * square

    def pass_on():
        for _, when, relay, arrival, _, _ in relays:

            def forward(arrival=arrival, relay=relay):
                arrival.wait_recv()
                relay.start()

            guarded(when, forward)

    def work(block):
        top = block * slots

        size = GROUPS[block]

        @pl.loop(0, slots // size)
        def _(group):
            base = pl.multiple_of(group * size, size)
            own_rows = recv_half[pl.ds(base, size), :].astype(bf16)
            near_rows = near[block, pl.ds(base, size), :].astype(bf16)
            for i in range(0, size, 2):
                edges = edges_of(own_rows[i : i + 2], near_rows[i : i + 2], send_half[top : top + slots, :], rel_half)
                sums = messages_of(dot(edges, pair_edge[...]), masked[top : top + slots, :])
                for n in range(2):
                    eight = pl.ds(pl.multiple_of((base + i + n) * 8, 8), 8)
                    part[eight, :] = part[eight, :] + sums[n] if block else sums[n]

            if block + 1 == RELAYED:
                pl.when(group == 0)(pass_on)

    for far in range(CLASSES):
        if has_mate and far == 0:
            mate_in.wait_recv()
        for step_far, when, _, arrival, _ in sends:
            if step_far == far and not (has_mate and far >= RELAYED):
                guarded(when, arrival.wait_recv)
        for step_far, when, _, _, twin_in, _ in relays:
            if step_far == far:
                guarded(when, twin_in.wait_recv)
        roles = [r for r, (_, step_far) in enumerate(lines) if step_far <= far]
        gather(roles, far * slots, room if far == CLASSES - 1 else (far + 1) * slots)
        if far < CLASSES - 1:
            work(far)
        if far == CLASSES - 2:
            pooled[...] = fold_rows(part, slots)

    for when, copy in [(s[1], s[2]) for s in sends] + [(r[1], r[2]) for r in relays]:
        guarded(when, copy.wait_send)
    if has_mate:
        mate_copy.wait_send()


B_LOADS = 5


def finish(*refs):
    send_half, near, recv_half, masked, pair_edge, pooled, tally = refs[:7]
    hbm, out_ref = refs[7 : 7 + B_LOADS], refs[7 + B_LOADS]
    held = refs[8 + B_LOADS : 8 + 2 * B_LOADS]
    load_sem, part = refs[8 + 2 * B_LOADS :]
    latents_ref, w_self, w_agg, w_out, norm_gain = held
    loads = [pltpu.make_async_copy(src, dst, load_sem.at[n]) for n, (src, dst) in enumerate(zip(hbm, held))]
    for load in loads:
        load.start()
    slots, width = recv_half.shape
    used = jnp.max(tally[:8, :]).astype(jnp.int32)
    steps = lax.div(used + (slots - 1), jnp.int32(slots)) * (slots // GROUPS[-1])
    part[...] = jnp.zeros_like(part)
    rel_half = tally[8:9, :].astype(bf16)

    @pl.loop(0, steps)
    def _(step):
        block, group = split(step, slots // GROUPS[-1])
        block = block + (CLASSES - 1)
        top = pl.multiple_of(block * slots, slots)
        base = pl.multiple_of(group * GROUPS[-1], GROUPS[-1])
        own_rows = recv_half[pl.ds(base, GROUPS[-1]), :].astype(bf16)
        near_rows = near[block, pl.ds(base, GROUPS[-1]), :].astype(bf16)
        for i in range(0, GROUPS[-1], 2):
            edges = edges_of(own_rows[i : i + 2], near_rows[i : i + 2], send_half[pl.ds(top, slots), :], rel_half)
            sums = messages_of(dot(edges, pair_edge[...]), masked[pl.ds(top, slots), :])
            for n in range(2):
                spot = pl.ds(pl.multiple_of((base + i + n) * 8, 8), 8)
                part[spot, :] = part[spot, :] + sums[n]

    for load in loads:
        load.wait()
    latent = latents_ref[0, 0, 0]
    mean = ((pooled[...] + fold_rows(part, slots)) / slots).astype(bf16)
    hidden = jax.nn.silu(dot(latent, w_self[0]) + dot(mean, w_agg[0])).astype(bf16)
    result = dot(hidden, w_out[0])
    center = jnp.mean(result, axis=-1, keepdims=True)
    shifted = result - center
    spread = jnp.mean(shifted * shifted, axis=-1, keepdims=True)
    normed = shifted * lax.rsqrt(spread + 1e-05) * norm_gain[...]
    out_ref[0, 0, 0] = (latent.astype(f32) + normed).astype(bf16)


def pinned(value):
    return pltpu.with_memory_space_constraint(value, pltpu.HBM)


def shards(
    latents, offsets, neighbours, counts, w_recv, w_send, w_rel, b_first, w_edge, b_edge, w_self, w_agg, w_out, norm_gain
):
    slots, width = latents.shape[3:]
    senders = neighbours.shape[3]
    room = senders + (CLASSES - 1) * slots
    spans = [slots_of(axis) for axis in AXES]
    count = spans[0] * spans[1] * spans[2]
    vmem = pl.BlockSpec(memory_space=pltpu.VMEM)
    far = pl.BlockSpec(memory_space=pltpu.HBM)
    args = (counts, latents, offsets, neighbours, w_recv, w_send, w_rel, b_first, w_edge, b_edge)
    between = (
        ((room, width), bf16), ((room // slots, slots, slots), f32), ((slots, width), f32), ((room, width), bf16),
        ((2 * width, 2 * width), bf16), ((slots, width), f32), ((16, slots), f32),
    )
    found = pl.pallas_call(
        exchange,
        out_shape=[jax.ShapeDtypeStruct(*s) for s in between],
        in_specs=[far] * A_INPUTS,
        out_specs=[vmem] * A_OUTPUTS,
        scratch_shapes=[pltpu.VMEM(v.shape, v.dtype) for v in args]
        + [
            pltpu.SemaphoreType.DMA((A_INPUTS,)),
            pltpu.VMEM((count, slots + PACK, width), bf16),
            pltpu.VMEM((count // spans[2], room, slots * spans[2]), bf16),
            pltpu.VMEM((slots * 8, width), f32),
            pltpu.SemaphoreType.DMA((18,)),
            pltpu.SemaphoreType.DMA((9,)),
            pltpu.SemaphoreType.DMA((count,)),
        ],
        compiler_params=pltpu.CompilerParams(
            collective_id=0, has_side_effects=True, vmem_limit_bytes=24 * 1024 * 1024
        ),
    )(args[0], *[pinned(v) for v in args[1:]])
    rest = tuple(pinned(v) for v in (latents, w_self, w_agg, w_out, norm_gain))
    return pl.pallas_call(
        finish,
        out_shape=jax.ShapeDtypeStruct(latents.shape, latents.dtype),
        in_specs=[vmem] * A_OUTPUTS + [far] * B_LOADS,
        out_specs=vmem,
        scratch_shapes=[pltpu.VMEM(v.shape, v.dtype) for v in rest]
        + [pltpu.SemaphoreType.DMA((B_LOADS,)), pltpu.VMEM((slots * 8, width), f32)],
        compiler_params=pltpu.CompilerParams(vmem_limit_bytes=24 * 1024 * 1024),
    )(*found, *rest)


def solution(mesh):
    cells = ("groups", "gx"), "gy", "gz"
    in_specs = (P(*cells, None, None), P(*cells, None, None), P(*cells, None), P(*cells))
    in_specs += (P(),) * 10
    return jax.shard_map(
        shards, mesh=mesh, in_specs=in_specs, out_specs=P(*cells, None, None), check_vma=False
    )
```

```python
import functools

import jax
import jax.numpy as jnp
from jax import lax
from jax.experimental import pallas as pl
from jax.experimental.pallas import tpu as pltpu
from jax.sharding import PartitionSpec as P

MESH = pl.DeviceIdType.MESH
AXES = ("gx", "gy", "gz")
PACK = 16
GROUPS = (128, 64, 128)
CLASSES = 3
RELAYED = 2
NT = (((1,), (1,)), ((), ()))
f32, bf16 = jnp.float32, jnp.bfloat16


def split(value, size):
    if size & (size - 1) == 0:
        return value >> (size.bit_length() - 1), value & (size - 1)
    return lax.div(value, size), lax.rem(value, size)


def wide(axis):
    return lax.axis_size(axis) > 2


def slots_of(axis):
    return min(lax.axis_size(axis), 3)


def moves(axis):
    size, here = lax.axis_size(axis), lax.axis_index(axis)
    if size == 1:
        return []
    if size == 2:
        return [(1 - here, None)]
    return [(here - 1, here > 0), (here + 1, here < size - 1)]


def slot_on(axis, source, target):
    return source - target + 1 if wide(axis) else source


def both(*conditions):
    held = [c for c in conditions if c is not None]
    return functools.reduce(jnp.logical_and, held) if held else None


def guarded(condition, action):
    if condition is None:
        action()
    else:
        pl.when(condition)(action)


def dot(a, b):
    return jnp.dot(a, b, preferred_element_type=f32)


def dot_nt(a, b):
    return lax.dot_general(a, b, NT, preferred_element_type=f32)


def edges_of(own, near, send, rel_half):
    halves = []
    for n in range(2):
        gap = jnp.transpose(jnp.broadcast_to(near[n : n + 1], (send.shape[1], send.shape[0])))
        pre = (own[n : n + 1] + send) + gap * rel_half
        halves.append(pre * (jnp.tanh(pre) + 1))
    return jnp.concatenate(halves, axis=1)


def messages_of(result, masked):
    width = masked.shape[1]
    half, sums = result.astype(bf16), []
    for n in range(2):
        total = None
        for r in range(0, masked.shape[0], PACK):
            msg = half[r : r + PACK, n * width : (n + 1) * width] + masked[r : r + PACK]
            gate = jnp.tanh(msg) + 1
            term = msg.astype(f32) * gate.astype(f32)
            total = term if total is None else total + term
        sums.append(total[:8] + total[8:])
    return sums


def fold_rows(part, rows):
    total = part[pl.ds(0, rows, stride=8), :]
    for k in range(1, 8):
        total = total + part[pl.ds(k, rows, stride=8), :]
    return total


A_INPUTS = 10
A_OUTPUTS = 7
LOAD_ORDER = (1, 5, 2, 6, 3, 0, 4, 7, 8, 9)


def exchange(*refs):
    hbm, outs = refs[:A_INPUTS], refs[A_INPUTS : A_INPUTS + A_OUTPUTS]
    held = refs[A_INPUTS + A_OUTPUTS : 2 * A_INPUTS + A_OUTPUTS]
    load_sem, table, chosen, part, send_sem, relay_sem, recv_sem = refs[2 * A_INPUTS + A_OUTPUTS :]
    counts_ref, latents_ref, offsets_ref, neighbours_ref, w_recv, w_send, w_rel, b_first, w_edge, b_edge = held
    send_half, near, recv_half, masked, pair_edge, pooled, tally = outs
    loads = [pltpu.make_async_copy(src, dst, load_sem.at[n]) for n, (src, dst) in enumerate(zip(hbm, held))]
    for n in LOAD_ORDER:
        loads[n].start()
    slots, width = latents_ref.shape[3], latents_ref.shape[4]
    senders = neighbours_ref.shape[3]
    blocks, room = senders // slots, senders + (CLASSES - 1) * slots
    here = [lax.axis_index(axis) for axis in AXES]
    sizes = [lax.axis_size(axis) for axis in AXES]
    spans = [slots_of(axis) for axis in AXES]
    count, span_z = table.shape[0], spans[2]

    def slot(coords):
        return (coords[0] * spans[1] + coords[1]) * spans[2] + coords[2]

    def slot_between(source, target):
        return slot([slot_on(a, s, t) for a, s, t in zip(AXES, source, target)])

    own = slot_between(here, here)
    own_line = own // span_z
    choices = [[(h, None, 0)] + [(v, when, 1) for v, when in moves(a)] for a, h in zip(AXES[:2], here)]
    routes = []
    for x, when_x, far_x in choices[0]:
        for y, when_y, far_y in choices[1]:
            if far_x + far_y:
                routes.append((far_x + far_y, (x, y, here[2]), both(when_x, when_y)))
    routes.sort(key=lambda r: r[0])
    has_mate = sizes[2] > 1
    mate = (here[0], here[1], 1 - here[2])

    def device(there):
        return dict(zip(AXES, there))

    barrier = pltpu.get_barrier_semaphore()

    def hello(there):
        pl.semaphore_signal(barrier, inc=1, device_id=device(there), device_id_type=MESH)

    if has_mate:
        hello(mate)
    for far, there, when in routes:
        guarded(when, functools.partial(hello, there))
        if has_mate and far < RELAYED:
            guarded(when, functools.partial(hello, (there[0], there[1], mate[2])))

    for n in (1, 5, 2, 6):
        loads[n].wait()
    latent = latents_ref[0, 0, 0]
    place = offsets_ref[0, 0, 0].astype(f32)
    rel = w_rel[0].astype(f32)
    rows = lax.broadcasted_iota(jnp.int32, (PACK, slots), 0)
    extra = jnp.zeros((PACK, slots), f32)
    for c in range(3):
        extra = jnp.where(rows == c, place[c : c + 1, :], extra)
        extra = jnp.where(rows == 3 + c, here[c].astype(f32), extra)
    col_ids = lax.broadcasted_iota(jnp.int32, (slots, slots), 0)
    spread = jnp.zeros((slots, slots), f32)
    rel_rows = jnp.zeros((slots, width), f32)
    for c in range(3):
        spread = jnp.where(col_ids == c, place[c : c + 1, :], spread)
        rel_rows = jnp.where(col_ids == c, rel[c : c + 1, :], rel_rows)
    rel_rows = rel_rows.astype(bf16)
    shift = dot(jnp.transpose(spread).astype(bf16), rel_rows)
    table[own, :slots, :] = (dot(latent, w_send[0]) + shift).astype(bf16)
    table[own, slots:, :] = extra.astype(bf16)

    for n in (3, 0):
        loads[n].wait()
    ids = jnp.concatenate([neighbours_ref[0, 0][:, b * slots : (b + 1) * slots] for b in range(blocks)], axis=0)
    cell, at = split(ids, slots)
    cell, z = split(cell, sizes[2])
    x, y = split(cell, sizes[1])
    found = [v - h + 1 if wide(a) else v for a, v, h in zip(AXES, (x, y, z), here)]
    spot = slot(found)
    index = lax.broadcasted_iota(jnp.int32, (blocks, slots), 0) * slots
    index = index + lax.broadcasted_iota(jnp.int32, (blocks, slots), 1)
    live = index < counts_ref[0]
    apart = sum(jnp.where(found[c] == slot_on(AXES[c], here[c], here[c]), 0, 1) for c in range(2))
    classes = [jnp.where(jnp.logical_and(live, apart == k), 1.0, 0.0) for k in range(CLASSES)]
    spare = -(CLASSES * blocks) % PACK
    marks = jnp.concatenate(classes + [jnp.zeros((spare, slots), f32)], axis=0).astype(bf16)
    a = lax.broadcasted_iota(jnp.int32, (slots, slots), 0)
    b = lax.broadcasted_iota(jnp.int32, (slots, slots), 1)
    ahead = jnp.concatenate([jnp.where(a < b, 1.0, 0.0), jnp.ones((slots, slots), f32)], axis=1).astype(bf16)
    ranks = dot(marks, ahead)
    goals = [jnp.full((1, slots), -1.0, f32)] * blocks
    base = jnp.zeros((1, slots), f32)
    for k in range(CLASSES):
        base = jnp.maximum(base, float(k * slots))
        for b in range(blocks):
            row = slice(k * blocks + b, k * blocks + b + 1)
            goals[b] = jnp.where(classes[k][b : b + 1] > 0, ranks[row, :slots] + base, goals[b])
            base = base + ranks[row, slots:]
    tally[:8, :] = jnp.broadcast_to(base - float((CLASSES - 1) * slots), (8, slots))
    tally[8:, :] = jnp.broadcast_to(0.5 * rel[3:4], (8, width))

    for n in (4, 7, 8, 9):
        loads[n].wait()
    order = lax.broadcasted_iota(jnp.int32, (room, slots), 0).astype(f32)
    picks, high, low = [], [], []
    for b in range(blocks):
        picks.append(jnp.where(order == goals[b], 1.0, 0.0).astype(bf16))
        high.append((spot[b : b + 1] * slots).astype(f32))
        low.append((at[b : b + 1] + 1).astype(f32))
    picks = jnp.concatenate(picks, axis=1)
    high = jnp.broadcast_to(jnp.concatenate(high, axis=1), (slots, senders)).astype(bf16)
    low = jnp.broadcast_to(jnp.concatenate(low, axis=1), (slots, senders)).astype(bf16)
    sorted_ids = dot_nt(picks, high) + dot_nt(picks, low)
    masked[...] = jnp.where(sorted_ids > 0.5, 0.5 * b_edge[...], -1e30).astype(bf16)
    sorted_ids = sorted_ids.astype(jnp.int32) - 1
    lanes = lax.broadcasted_iota(jnp.int32, (room, slots), 1)

    cell_x, cell_z = split(lax.broadcasted_iota(jnp.int32, (slots, slots), 0), spans[2])
    cell_x, cell_y = split(cell_x, spans[1])
    step = jnp.zeros((slots, width), f32)
    for c, v in enumerate((cell_x, cell_y, cell_z)):
        gap = v - 1 if wide(AXES[c]) else v - here[c]
        step = step + gap.astype(f32) * rel[c : c + 1]
    step_high = step.astype(bf16)
    step_low = (step - step_high.astype(f32)).astype(bf16)
    of_cell = jnp.where(lax.shift_right_arithmetic(sorted_ids, slots.bit_length() - 1) == lanes, 1.0, 0.0).astype(bf16)
    moved = dot(of_cell, step_high) + dot(of_cell, step_low)

    peers = jnp.int32(1 if has_mate else 0)
    for far, _, when in routes:
        cores = 2 if has_mate and far < RELAYED else 1
        peers = peers + (cores if when is None else cores * when.astype(jnp.int32))
    pl.semaphore_wait(barrier, peers)

    def remote(source, spot, sem, there):
        return pltpu.make_async_remote_copy(
            src_ref=table.at[source], dst_ref=table.at[spot], send_sem=sem, recv_sem=recv_sem.at[spot],
            device_id=device(there), device_id_type=MESH,
        )

    lines, sends, relays = [(own_line, 0)], [], []
    for far, there, when in routes:
        mine = slot_between(there, here)
        twin = slot_between((there[0], there[1], mate[2]), here)
        lines.append((mine // span_z, far))
        other = (there[0], there[1], mate[2])
        n = len(sends)
        sends.append((far, when, remote(own, slot_between(here, there), send_sem.at[n], there),
                      remote(own, mine, send_sem.at[n], there), mine))
        if not has_mate:
            continue
        if far < RELAYED:
            sends.append((far, when, remote(own, slot_between(here, other), send_sem.at[n + 1], other),
                          remote(own, twin, send_sem.at[n + 1], other), twin))
        else:
            n = len(relays)
            relays.append((far, when, remote(mine, mine, relay_sem.at[n], mate), sends[-1][3],
                           remote(own, twin, relay_sem.at[n], mate), twin))
    if has_mate:
        mate_own = slot_between(mate, here)
        mate_copy = remote(own, own, send_sem.at[len(sends)], mate)
        mate_in = remote(own, mate_own, send_sem.at[len(sends)], mate)
        mate_copy.start()
    for _, when, copy, _, _ in sends:
        guarded(when, copy.start)

    def clear(which):
        table[which] = jnp.zeros(table.shape[1:], bf16)

    for when, which in [(s[1], s[4]) for s in sends] + [(r[1], r[5]) for r in relays]:
        if when is not None:
            pl.when(jnp.logical_not(when))(functools.partial(clear, which))

    for r, (line, far) in enumerate(lines):
        for k in range(span_z):
            hit = sorted_ids[far * slots :] - (line * span_z + k) * slots == lanes[far * slots :]
            chosen[r, far * slots :, k * slots : (k + 1) * slots] = jnp.where(hit, 1.0, 0.0).astype(bf16)

    edge_half = 0.5 * w_edge[0].astype(f32)
    nil = jnp.zeros_like(edge_half)
    pair_edge[...] = jnp.concatenate(
        [jnp.concatenate([edge_half, nil], axis=1), jnp.concatenate([nil, edge_half], axis=1)], axis=0
    ).astype(bf16)
    rel_half = (0.5 * rel[3:4]).astype(bf16)
    recv_half[...] = 0.5 * (dot(latent, w_recv[0]) + b_first[...] - shift)
    place_cols = [jnp.transpose(jnp.broadcast_to(place[c : c + 1], (slots, slots))) for c in range(3)]

    def begin(top, bottom):
        return jnp.concatenate([moved[top:bottom], jnp.zeros((bottom - top, PACK), f32)], axis=1)

    def pick(roles, top, bottom, total):
        for r in roles:
            picked, cells = chosen[r, top:bottom, :], table.at[pl.ds(lines[r][0] * span_z, span_z)]
            sides = [jnp.transpose(cells[k, slots:, :].astype(f32)).astype(bf16) for k in range(span_z)]
            both_of = jnp.concatenate(
                [cells[:, :slots, :].reshape(span_z * slots, width), jnp.concatenate(sides, axis=0)], axis=1
            )
            total = total + dot(picked, both_of)
        return total

    def store(total, top, bottom):
        send_half[top:bottom, :] = (0.5 * total[:, :width]).astype(bf16)
        for n in range(top // slots, bottom // slots):
            feats = jnp.transpose(total[n * slots - top : (n + 1) * slots - top, width:])
            square = jnp.zeros((slots, slots), f32)
            for c in range(3):
                where = feats[c : c + 1] + (feats[3 + c : 4 + c] - here[c].astype(f32))
                gap = where - place_cols[c]
                square = square + gap * gap
            near[n] = 0.25 * square

    def pass_on():
        for _, when, relay, arrival, _, _ in relays:

            def forward(arrival=arrival, relay=relay):
                arrival.wait_recv()
                relay.start()

            guarded(when, forward)

    def work(block):
        top = block * slots

        size = GROUPS[block]

        @pl.loop(0, slots // size)
        def _(group):
            base = pl.multiple_of(group * size, size)
            own_rows = recv_half[pl.ds(base, size), :].astype(bf16)
            near_rows = near[block, pl.ds(base, size), :].astype(bf16)
            for i in range(0, size, 2):
                edges = edges_of(own_rows[i : i + 2], near_rows[i : i + 2], send_half[top : top + slots, :], rel_half)
                sums = messages_of(dot(edges, pair_edge[...]), masked[top : top + slots, :])
                for n in range(2):
                    eight = pl.ds(pl.multiple_of((base + i + n) * 8, 8), 8)
                    part[eight, :] = part[eight, :] + sums[n] if block else sums[n]

            if block + 1 == RELAYED:
                pl.when(group == 0)(pass_on)

    for far in range(CLASSES):
        top, bottom = far * slots, room if far == CLASSES - 1 else (far + 1) * slots
        total = pick([r for r, (_, step_far) in enumerate(lines) if step_far < far], top, bottom, begin(top, bottom))
        if has_mate and far == 0:
            mate_in.wait_recv()
        for step_far, when, _, arrival, _ in sends:
            if step_far == far and not (has_mate and far >= RELAYED):
                guarded(when, arrival.wait_recv)
        for step_far, when, _, _, twin_in, _ in relays:
            if step_far == far:
                guarded(when, twin_in.wait_recv)
        total = pick([r for r, (_, step_far) in enumerate(lines) if step_far == far], top, bottom, total)
        store(total, top, bottom)
        if far < CLASSES - 1:
            work(far)
        if far == CLASSES - 2:
            pooled[...] = fold_rows(part, slots)

    for when, copy in [(s[1], s[2]) for s in sends] + [(r[1], r[2]) for r in relays]:
        guarded(when, copy.wait_send)
    if has_mate:
        mate_copy.wait_send()


B_LOADS = 5


def finish(*refs):
    send_half, near, recv_half, masked, pair_edge, pooled, tally = refs[:7]
    hbm, out_ref = refs[7 : 7 + B_LOADS], refs[7 + B_LOADS]
    held = refs[8 + B_LOADS : 8 + 2 * B_LOADS]
    load_sem, part = refs[8 + 2 * B_LOADS :]
    latents_ref, w_self, w_agg, w_out, norm_gain = held
    loads = [pltpu.make_async_copy(src, dst, load_sem.at[n]) for n, (src, dst) in enumerate(zip(hbm, held))]
    for load in loads:
        load.start()
    slots, width = recv_half.shape
    used = jnp.max(tally[:8, :]).astype(jnp.int32)
    steps = lax.div(used + (slots - 1), jnp.int32(slots)) * (slots // GROUPS[-1])
    part[...] = jnp.zeros_like(part)
    rel_half = tally[8:9, :].astype(bf16)

    @pl.loop(0, steps)
    def _(step):
        block, group = split(step, slots // GROUPS[-1])
        block = block + (CLASSES - 1)
        top = pl.multiple_of(block * slots, slots)
        base = pl.multiple_of(group * GROUPS[-1], GROUPS[-1])
        own_rows = recv_half[pl.ds(base, GROUPS[-1]), :].astype(bf16)
        near_rows = near[block, pl.ds(base, GROUPS[-1]), :].astype(bf16)
        for i in range(0, GROUPS[-1], 2):
            edges = edges_of(own_rows[i : i + 2], near_rows[i : i + 2], send_half[pl.ds(top, slots), :], rel_half)
            sums = messages_of(dot(edges, pair_edge[...]), masked[pl.ds(top, slots), :])
            for n in range(2):
                spot = pl.ds(pl.multiple_of((base + i + n) * 8, 8), 8)
                part[spot, :] = part[spot, :] + sums[n]

    for load in loads:
        load.wait()
    latent = latents_ref[0, 0, 0]
    mean = ((pooled[...] + fold_rows(part, slots)) / slots).astype(bf16)
    hidden = jax.nn.silu(dot(latent, w_self[0]) + dot(mean, w_agg[0])).astype(bf16)
    result = dot(hidden, w_out[0])
    center = jnp.mean(result, axis=-1, keepdims=True)
    shifted = result - center
    spread = jnp.mean(shifted * shifted, axis=-1, keepdims=True)
    normed = shifted * lax.rsqrt(spread + 1e-05) * norm_gain[...]
    out_ref[0, 0, 0] = (latent.astype(f32) + normed).astype(bf16)


def pinned(value):
    return pltpu.with_memory_space_constraint(value, pltpu.HBM)


def shards(
    latents, offsets, neighbours, counts, w_recv, w_send, w_rel, b_first, w_edge, b_edge, w_self, w_agg, w_out, norm_gain
):
    slots, width = latents.shape[3:]
    senders = neighbours.shape[3]
    room = senders + (CLASSES - 1) * slots
    spans = [slots_of(axis) for axis in AXES]
    count = spans[0] * spans[1] * spans[2]
    vmem = pl.BlockSpec(memory_space=pltpu.VMEM)
    far = pl.BlockSpec(memory_space=pltpu.HBM)
    args = (counts, latents, offsets, neighbours, w_recv, w_send, w_rel, b_first, w_edge, b_edge)
    between = (
        ((room, width), bf16), ((room // slots, slots, slots), f32), ((slots, width), f32), ((room, width), bf16),
        ((2 * width, 2 * width), bf16), ((slots, width), f32), ((16, slots), f32),
    )
    found = pl.pallas_call(
        exchange,
        out_shape=[jax.ShapeDtypeStruct(*s) for s in between],
        in_specs=[far] * A_INPUTS,
        out_specs=[vmem] * A_OUTPUTS,
        scratch_shapes=[pltpu.VMEM(v.shape, v.dtype) for v in args]
        + [
            pltpu.SemaphoreType.DMA((A_INPUTS,)),
            pltpu.VMEM((count, slots + PACK, width), bf16),
            pltpu.VMEM((count // spans[2], room, slots * spans[2]), bf16),
            pltpu.VMEM((slots * 8, width), f32),
            pltpu.SemaphoreType.DMA((18,)),
            pltpu.SemaphoreType.DMA((9,)),
            pltpu.SemaphoreType.DMA((count,)),
        ],
        compiler_params=pltpu.CompilerParams(
            collective_id=0, has_side_effects=True, vmem_limit_bytes=24 * 1024 * 1024
        ),
    )(args[0], *[pinned(v) for v in args[1:]])
    rest = tuple(pinned(v) for v in (latents, w_self, w_agg, w_out, norm_gain))
    return pl.pallas_call(
        finish,
        out_shape=jax.ShapeDtypeStruct(latents.shape, latents.dtype),
        in_specs=[vmem] * A_OUTPUTS + [far] * B_LOADS,
        out_specs=vmem,
        scratch_shapes=[pltpu.VMEM(v.shape, v.dtype) for v in rest]
        + [pltpu.SemaphoreType.DMA((B_LOADS,)), pltpu.VMEM((slots * 8, width), f32)],
        compiler_params=pltpu.CompilerParams(vmem_limit_bytes=24 * 1024 * 1024),
    )(*found, *rest)


def solution(mesh):
    cells = ("groups", "gx"), "gy", "gz"
    in_specs = (P(*cells, None, None), P(*cells, None, None), P(*cells, None), P(*cells))
    in_specs += (P(),) * 10
    return jax.shard_map(
        shards, mesh=mesh, in_specs=in_specs, out_specs=P(*cells, None, None), check_vma=False
    )
```
